32 devices in a mesh: dp: 1 (over z), tp: 32 (over y, x, core).
Axes of the slice: x: 4, y: 4, z: 1, core: 2. Of those that a mesh axis runs over, the one named last changes fastest.
The devices are a block of a 4x4x8 slice.
Arguments:
- hidden: bfloat16 [2048, 2048], P('dp')
- w_query: bfloat16 [2048, 2048], P(None, 'tp')
- w_key: bfloat16 [2048, 128], replicated
- w_value: bfloat16 [2048, 128], replicated
- w_out: bfloat16 [2048, 2048], P('tp')
- k_cache: bfloat16 [2048, 256, 128], P(('dp', 'tp'))
- v_cache: bfloat16 [2048, 256, 128], P(('dp', 'tp'))
- lengths: int32 [2048], P('dp')
Outputs:
- output 1: bfloat16 [2048, 2048], P('dp', 'tp')
- output 2: bfloat16 [2048, 256, 128], P(('dp', 'tp'))
- output 3: bfloat16 [2048, 256, 128], P(('dp', 'tp'))
All inputs are finite; a program needn't handle non-finite values.
Results may differ from the reference program's by a relative error of at most 0.0145829.
Values are sent between devices in bfloat16 or wider.
A program may use at most 768 MiB of HBM per device.

```python
import jax
import jax.numpy as jnp
from jax import lax

BATCH_ROWS = 2048
EMBED_DIM = 2048
Q_HEADS = 16
HEAD_DIM = 128
SEQ_LEN = 256


def setup_inputs(seed: int = 0, part: int = 0) -> dict:
    part_key = jax.random.fold_in(jax.random.key(seed), part)
    key_hid, key_kc, key_vc, key_mean, key_len, key_top = jax.random.split(part_key, 6)
    weight_keys = jax.random.split(jax.random.key(seed + 1), 4)
    total_cols = Q_HEADS * HEAD_DIM
    hidden = jax.random.normal(key_hid, (BATCH_ROWS, EMBED_DIM), jnp.float32)
    w_query = jax.random.normal(weight_keys[0], (EMBED_DIM, total_cols), jnp.float32) * EMBED_DIM ** -0.5
    w_key = jax.random.normal(weight_keys[1], (EMBED_DIM, HEAD_DIM), jnp.float32) * (2.5 * EMBED_DIM ** -0.5)
    w_value = jax.random.normal(weight_keys[2], (EMBED_DIM, HEAD_DIM), jnp.float32) * EMBED_DIM ** -0.5
    w_out = jax.random.normal(weight_keys[3], (total_cols, EMBED_DIM), jnp.float32) * total_cols ** -0.5
    k_cache = 2.5 * jax.random.normal(key_kc, (BATCH_ROWS, SEQ_LEN, HEAD_DIM), jnp.float32)
    v_mean = 0.5 * jax.random.normal(key_mean, (BATCH_ROWS, 1, HEAD_DIM), jnp.float32)
    v_cache = v_mean + jax.random.normal(key_vc, (BATCH_ROWS, SEQ_LEN, HEAD_DIM), jnp.float32)
    drawn_len = jax.random.randint(key_len, (BATCH_ROWS,), 0, SEQ_LEN)
    top_row = jax.random.randint(key_top, (), 0, BATCH_ROWS)
    lengths = jnp.where(jnp.arange(BATCH_ROWS) == top_row, SEQ_LEN - 1, drawn_len).astype(jnp.int32)
    return {
        'hidden': hidden.astype(jnp.bfloat16),
        'w_query': w_query.astype(jnp.bfloat16),
        'w_key': w_key.astype(jnp.bfloat16),
        'w_value': w_value.astype(jnp.bfloat16),
        'w_out': w_out.astype(jnp.bfloat16),
        'k_cache': k_cache.astype(jnp.bfloat16),
        'v_cache': v_cache.astype(jnp.bfloat16),
        'lengths': lengths,
    }


def rope_angles(positions):
    half_dim = HEAD_DIM // 2
    inv_freq = 10000.0 ** (-(jnp.arange(half_dim, dtype=jnp.float32) * 2.0) / HEAD_DIM)
    return positions.astype(jnp.float32)[:, None] * inv_freq[None, :]


def apply_rope(values_in, angles):
    half_dim = values_in.shape[-1] // 2
    first_half = values_in[..., :half_dim]
    second_half = values_in[..., half_dim:]
    cosines = jnp.cos(angles)
    sines = jnp.sin(angles)
    return jnp.concatenate([first_half * cosines - second_half * sines, second_half * cosines + first_half * sines], axis=-1)


def attend_row(row_args):
    q_row, k_row, v_row, length = row_args
    scores = jnp.dot(q_row, k_row.T, preferred_element_type=jnp.float32) * (HEAD_DIM ** -0.5)
    valid_mask = jnp.arange(SEQ_LEN)[None, :] <= length
    scores = jnp.where(valid_mask, scores, -1e30)
    row_max = jnp.max(scores, axis=-1, keepdims=True)
    weights = jnp.exp(scores - row_max)
    denominator = jnp.sum(weights, axis=-1, keepdims=True)
    summed = jnp.dot(weights.astype(jnp.bfloat16), v_row, preferred_element_type=jnp.float32)
    return (summed / denominator).astype(jnp.bfloat16)


def reference(hidden, w_query, w_key, w_value, w_out, k_cache, v_cache, lengths):
    q_flat = jnp.dot(hidden, w_query, preferred_element_type=jnp.float32).astype(jnp.bfloat16)
    k_new = jnp.dot(hidden, w_key, preferred_element_type=jnp.float32).astype(jnp.bfloat16)
    v_new = jnp.dot(hidden, w_value, preferred_element_type=jnp.float32).astype(jnp.bfloat16)
    angles = rope_angles(lengths)
    q_heads = q_flat.reshape(BATCH_ROWS, Q_HEADS, HEAD_DIM).astype(jnp.float32)
    q_rot = apply_rope(q_heads, angles[:, None, :]).astype(jnp.bfloat16)
    k_rot = apply_rope(k_new.astype(jnp.float32), angles).astype(jnp.bfloat16)
    new_slot = (jnp.arange(SEQ_LEN)[None, :] == lengths[:, None])[:, :, None]
    k_cache_out = jnp.where(new_slot, k_rot[:, None, :], k_cache)
    v_cache_out = jnp.where(new_slot, v_new[:, None, :], v_cache)
    attn_out = lax.map(attend_row, (q_rot, k_cache_out, v_cache_out, lengths))
    y_out = jnp.dot(attn_out.reshape(BATCH_ROWS, Q_HEADS * HEAD_DIM), w_out, preferred_element_type=jnp.float32).astype(jnp.bfloat16)
    return (y_out, k_cache_out, v_cache_out)
```

```python
import functools
import math

import jax
import jax.numpy as jnp
from jax import lax
from jax.experimental import pallas as pl
from jax.experimental.pallas import tpu as pltpu
from jax.sharding import PartitionSpec as P

F32, BF16 = jnp.float32, jnp.bfloat16
MESH = pl.DeviceIdType.MESH
TILE = 16
CACHE_STEPS = 8
O_STEPS = 4


def rope_tables(positions, head_dim):
    half_dim = head_dim // 2
    inv_freq = 10000.0 ** (-(jnp.arange(half_dim, dtype=F32) * 2.0) / head_dim)
    angles = positions.astype(F32)[:, None] * inv_freq[None, :]
    return jnp.cos(angles), jnp.sin(angles)


def cache_kernel(lens, hidden, w_key, w_value, cos, sin, k_in, v_in, k_out, v_out,
                 k_buf, v_buf, h_buf, wk_buf, wv_buf, k_new, v_new, in_sem, out_sem, small_sem):
    rows, seq, dim = k_in.shape
    step_rows = rows // CACHE_STEPS
    first = lax.axis_index("tp") * rows
    small = [
        pltpu.make_async_copy(hidden.at[pl.ds(first, rows)], h_buf, small_sem.at[0]),
        pltpu.make_async_copy(w_key, wk_buf, small_sem.at[1]),
        pltpu.make_async_copy(w_value, wv_buf, small_sem.at[2]),
    ]
    for copy in small:
        copy.start()
    pairs = ((k_in, k_buf, k_out), (v_in, v_buf, v_out))
    ins, outs = [], []
    for j in range(CACHE_STEPS):
        part = pl.ds(j * step_rows, step_rows)
        ins.append([pltpu.make_async_copy(src.at[part], buf.at[part], in_sem.at[i, j]) for i, (src, buf, _) in enumerate(pairs)])
        outs.append([pltpu.make_async_copy(buf.at[part], dst.at[part], out_sem.at[i, j]) for i, (_, buf, dst) in enumerate(pairs)])
        for copy in ins[j]:
            copy.start()
    for copy in small:
        copy.wait()
    half = dim // 2
    key = jnp.dot(h_buf[...], wk_buf[...], preferred_element_type=F32).astype(BF16).astype(F32)
    x1, x2, c, s = key[:, :half], key[:, half:], cos[...], sin[...]
    k_new[...] = jnp.concatenate([x1 * c - x2 * s, x2 * c + x1 * s], axis=1)
    v_new[...] = jnp.dot(h_buf[...], wv_buf[...], preferred_element_type=F32)
    slot = lax.broadcasted_iota(jnp.int32, (TILE, dim), 0)
    for j in range(CACHE_STEPS):
        for copy in ins[j]:
            copy.wait()
        for r in range(j * step_rows, (j + 1) * step_rows):
            position = lens[r]
            start = pl.multiple_of((position // TILE) * TILE, TILE)
            here = slot == position - start
            for buf, new in ((k_buf, k_new), (v_buf, v_new)):
                old = buf[r, pl.ds(start, TILE), :].astype(F32)
                buf[r, pl.ds(start, TILE), :] = jnp.where(here, new[pl.ds(r, 1), :], old).astype(BF16)
        for copy in outs[j]:
            copy.start()
    for step in outs:
        for copy in step:
            copy.wait()


def step_kernel(side, hidden, w_query, w_out, k_all, v_all, lens, cos, sin, y_out,
                h_buf, wq_buf, wo_buf, w_buf, k_buf, v_buf, q_send, q_recv, q_rows, o_rows, o_buf,
                y_send, y_recv,
                h_sem, wq_sem, wo_sem, k_sem, v_sem, q_ssem, q_rsem, w_ssem, w_rsem, o_ssem, o_rsem, y_ssem, y_rsem):
    rows, seq, dim = k_all.shape
    half = dim // 2
    pack = rows // 2
    group = 2 * side * side
    heads = group // 2
    cols = w_buf.shape[1]
    me = lax.axis_index("tp")
    core = lax.rem(me, 2)
    chip = me // 2
    x = lax.rem(chip, side)
    y = chip // side

    def index(xx, yy, cc):
        return (lax.rem(yy, side) * side + lax.rem(xx, side)) * 2 + cc

    def remote(src, dst, ssem, rsem, target):
        return pltpu.make_async_remote_copy(src_ref=src, dst_ref=dst, send_sem=ssem, recv_sem=rsem,
                                            device_id={"tp": target}, device_id_type=MESH)

    block = rows * 2 * side
    ydest = [lax.rem(y + d, side) for d in (2, 1, 3, 0)]

    def h_part(yy):
        return pl.ds(pl.multiple_of(yy * block, block), block)

    wq_copy = pltpu.make_async_copy(w_query, wq_buf, wq_sem)
    wq_copy.start()
    h_copies = [pltpu.make_async_copy(hidden.at[h_part(yy)], h_buf.at[h_part(yy)], h_sem.at[i]) for i, yy in enumerate(ydest)]
    for copy in h_copies:
        copy.start()
    wo_copies = []
    for i in range(side):
        wo_copies.append(pltpu.make_async_copy(w_out.at[:, pl.ds(i * cols, cols)], wo_buf.at[i], wo_sem.at[i]))
        wo_copies[i].start()
    step_rows = rows // O_STEPS
    kv_copies = []
    for k in range(O_STEPS):
        part = pl.ds(k * step_rows, step_rows)
        kv_copies.append((pltpu.make_async_copy(k_all.at[part], k_buf.at[part], k_sem.at[k]),
                          pltpu.make_async_copy(v_all.at[part], v_buf.at[part], v_sem.at[k])))
        for copy in kv_copies[k]:
            copy.start()

    barrier = pltpu.get_barrier_semaphore()
    peers = [(lax.rem(chip + i, heads)) * 2 + c for i in range(1, heads) for c in range(2)] + [chip * 2 + (1 - core)]
    for peer in peers:
        pl.semaphore_signal(barrier, inc=1, device_id={"tp": peer}, device_id_type=MESH)

    wq_copy.wait()
    sends = []
    for i, yy in enumerate(ydest):
        h_copies[i].wait()
        q_val = jnp.dot(h_buf[h_part(yy), :], wq_buf[...], preferred_element_type=F32).astype(BF16)
        q_val = q_val.reshape(2 * side, 2, pack, half)
        q_send[i] = jnp.concatenate([q_val[:, 0], q_val[:, 1]], axis=-1)
        if i == 0:
            pl.semaphore_wait(barrier, len(peers))

        def send_q(j, carry, i=i, yy=yy):
            slot = lax.rem(j + x * 2 + 2, 2 * side)
            target = yy * 2 * side + slot
            remote(q_send.at[i, slot], q_recv.at[me], q_ssem.at[i * 2 * side + slot], q_rsem.at[me], target).start()
            return carry

        if i < side - 1:
            lax.fori_loop(0, 2 * side, send_q, 0)
        else:
            own = x * 2 + core

            def send_own_row(j, carry, i=i, yy=yy):
                slot = lax.rem(own + 1 + j, 2 * side)
                target = yy * 2 * side + slot
                remote(q_send.at[i, slot], q_recv.at[me], q_ssem.at[i * 2 * side + slot], q_rsem.at[me], target).start()
                return carry

            lax.fori_loop(0, 2 * side - 1, send_own_row, 0)
            q_recv[me] = q_send[i, own]

    def w_slot(t):
        return w_buf.at[pl.ds(pl.multiple_of(t * half, half), half)]

    for copy in wo_copies:
        copy.wait()
    n_w = [0]

    def send_w(src, t, target):
        copy = remote(src, w_slot(t), w_ssem.at[n_w[0]], w_rsem.at[t], target)
        n_w[0] += 1
        copy.start()
        sends.append(copy)

    def wait_w(t):
        remote(w_slot(t), w_slot(t), w_ssem.at[0], w_rsem.at[t], me).wait_recv()

    w_buf[pl.ds(pl.multiple_of(me * half, half), half)] = wo_buf[y]
    for d in (1, 3, 2):
        send_w(wo_buf.at[lax.rem(y + d, side)], me, index(x, y + d, core))
    left, right, other = index(x + side - 1, y, core), index(x + 1, y, core), chip * 2 + (1 - core)
    for target in (right, left, other):
        send_w(wo_buf.at[y], me, target)

    def forward_column(d):
        t = index(x, y + d, core)
        wait_w(t)
        for target in (right, left, other):
            send_w(w_slot(t), t, target)

    for d in (1, 3, 2):
        forward_column(d)

    lane = lax.broadcasted_iota(jnp.int32, (pack, dim), 1) < half
    c_low, c_high = cos[pl.ds(0, pack), :], cos[pl.ds(pack, pack), :]
    s_low, s_high = sin[pl.ds(0, pack), :], sin[pl.ds(pack, pack), :]
    c_pack = jnp.concatenate([c_low, c_high], axis=1)
    s_pack = jnp.concatenate([s_low, s_high], axis=1)
    for i in range(1, group):
        t = lax.rem(me + i, group)
        remote(q_recv.at[t], q_recv.at[t], q_ssem.at[0], q_rsem.at[t], me).wait_recv()
    for i in range(heads):
        p1, p2 = q_recv[2 * i].astype(F32), q_recv[2 * i + 1].astype(F32)
        r1, r2 = p1 * c_pack - p2 * s_pack, p2 * c_pack + p1 * s_pack
        q_rows[pl.ds(i, pack, stride=heads), :] = jnp.where(lane, r1, pltpu.roll(r2, half, 1))
        q_rows[pl.ds(pack * heads + i, pack, stride=heads), :] = jnp.where(lane, pltpu.roll(r1, half, 1), r2)

    def relay_right(d):
        t = index(x + side - 1, y + d, core)
        wait_w(t)
        send_w(w_slot(t), t, right)
        send_w(w_slot(t), t, other)

    def relay_left(d):
        t = index(x + 1, y + d, core)
        wait_w(t)
        send_w(w_slot(t), t, left)
        send_w(w_slot(t), t, other)

    def pass_on(xx, d):
        t = index(xx, y + d, core)
        wait_w(t)
        send_w(w_slot(t), t, other)

    scale = dim ** -0.5
    slots = lax.broadcasted_iota(jnp.int32, (heads, seq), 1)
    up, down = index(x, y + 1, core), index(x, y + side - 1, core)
    y_up, y_down, y_far = lax.rem(y + 1, side), lax.rem(y + side - 1, side), lax.rem(y + 2, side)
    n_o = [0]

    def send_o(yy, k, target):
        copy = remote(o_buf.at[yy, k], o_buf.at[yy, k], o_ssem.at[n_o[0]], o_rsem.at[yy, k], target)
        n_o[0] += 1
        copy.start()
        sends.append(copy)

    def wait_o(yy, k):
        remote(o_buf.at[yy, k], o_buf.at[yy, k], o_ssem.at[0], o_rsem.at[yy, k], me).wait_recv()

    def relay_o(k):
        if k % 2 == 0:
            wait_o(y_down, k)
            send_o(y_down, k, up)
        else:
            wait_o(y_up, k)
            send_o(y_up, k, down)

    def attend(k):
        for copy in kv_copies[k]:
            copy.wait()

        def some_rows(j, carry):
            for u in range(8):
                part = j * 8 + u
                r = k * step_rows + part
                q_row = q_rows[pl.ds(pl.multiple_of(r * heads, heads), heads), :].astype(BF16)
                scores = lax.dot_general(q_row, k_buf[r], (((1,), (1,)), ((), ())), preferred_element_type=F32) * scale
                scores = jnp.where(slots <= lens[pl.ds(r, 1), :], scores, -1e30)
                weights = jnp.exp(scores - jnp.max(scores, axis=1, keepdims=True))
                total = jnp.sum(weights, axis=1, keepdims=True)
                summed = jnp.dot(weights.astype(BF16), v_buf[r], preferred_element_type=F32)
                o_rows[pl.ds(pl.multiple_of(part * heads, heads), heads), :] = summed / total
            return carry

        lax.fori_loop(0, step_rows // 8, some_rows, 0)
        for i in range(heads):
            o_buf[y, k, i] = o_rows[pl.ds(i, step_rows, stride=heads), :].astype(BF16)
        send_o(y, k, up)
        send_o(y, k, down)

    attend(0)
    relay_right(0)
    relay_left(3)
    attend(1)
    relay_right(1)
    relay_left(2)
    pass_on(x + side - 1, 2)
    pass_on(x + side - 1, 3)
    attend(2)
    relay_o(0)
    pass_on(x + 1, 0)
    pass_on(x + 1, 1)
    attend(3)
    relay_o(1)
    for d in (0, 3, 1, 2):
        pass_on(x + 2, d)
    for i in range(heads):
        wait_w(2 * i + 1 - core)

    y_sends = []

    def project(yy):
        lhs = jnp.concatenate([o_buf[yy, :, i].reshape(rows, dim) for i in range(heads)], axis=1)
        res = jnp.dot(lhs, w_buf[...], preferred_element_type=F32).astype(BF16)
        row_owner = index(x, yy, core)
        n = len(y_sends)
        y_sends.append(yy)
        for slot in range(2 * side):
            part = res[:, slot * half:(slot + 1) * half]
            y_send[n, slot] = jnp.concatenate([part[:pack], part[pack:]], axis=1)
        own = x * 2 + core

        def send_y(j, carry):
            slot = lax.rem(own + 1 + j, 2 * side)
            target = y * 2 * side + slot
            remote(y_send.at[n, slot], y_recv.at[row_owner], y_ssem.at[n * 2 * side + slot], y_rsem.at[row_owner], target).start()
            return carry

        lax.fori_loop(0, 2 * side - 1, send_y, 0)
        y_recv[row_owner] = y_send[n, own]

    project(y)
    relay_o(2)
    relay_o(3)
    wait_o(y_up, 0)
    wait_o(y_up, 2)
    project(y_up)
    wait_o(y_down, 1)
    wait_o(y_down, 3)
    project(y_down)
    for k in range(O_STEPS):
        wait_o(y_far, k)
    project(y_far)

    own = x * 2 + core
    for yy in (y, y_up, y_down, y_far):
        def wait_y(j, carry, yy=yy):
            slot = lax.rem(own + 1 + j, 2 * side)
            t = yy * 2 * side + slot
            remote(y_recv.at[t], y_recv.at[t], y_ssem.at[0], y_rsem.at[t], me).wait_recv()
            return carry

        lax.fori_loop(0, 2 * side - 1, wait_y, 0)
    y_out[...] = y_recv[...]

    for copy in sends:
        copy.wait_send()

    def drain_q(j, carry):
        i, slot = j // (2 * side), lax.rem(j, 2 * side)
        remote(q_send.at[i, slot], q_recv.at[me], q_ssem.at[j], q_rsem.at[me], me).wait_send()
        return carry

    lax.fori_loop(0, (side - 1) * 2 * side, drain_q, 0)

    def drain_own(j, carry):
        slot = lax.rem(own + 1 + j, 2 * side)
        i = side - 1
        remote(q_send.at[i, slot], q_recv.at[me], q_ssem.at[i * 2 * side + slot], q_rsem.at[me], me).wait_send()
        for n in range(side):
            remote(y_send.at[n, slot], y_recv.at[me], y_ssem.at[n * 2 * side + slot], y_rsem.at[me], me).wait_send()
        return carry

    lax.fori_loop(0, 2 * side - 1, drain_own, 0)


def solution(mesh):
    group = mesh.shape["tp"]
    side = math.isqrt(group // 2)
    cache_spec = P(("dp", "tp"), None, None)
    vmem, hbm = pl.BlockSpec(memory_space=pltpu.VMEM), pl.BlockSpec(memory_space=pl.ANY)
    smem = pl.BlockSpec(memory_space=pltpu.SMEM)
    dma = pltpu.SemaphoreType.DMA

    def local_step(hidden, w_query, w_key, w_value, w_out, k_cache, v_cache, lengths):
        rows, seq, dim = k_cache.shape
        batch, embed = hidden.shape
        half = dim // 2
        heads = group * w_query.shape[1] // dim
        cols = w_out.shape[1] // side
        own_lengths = lax.dynamic_slice_in_dim(lengths, lax.axis_index("tp") * rows, rows, axis=0)
        cos, sin = rope_tables(own_lengths, dim)
        lens = jnp.broadcast_to(own_lengths[:, None], (rows, seq))
        cache_shape = jax.ShapeDtypeStruct(k_cache.shape, k_cache.dtype)
        k_out, v_out = pl.pallas_call(
            cache_kernel,
            out_shape=(cache_shape, cache_shape),
            in_specs=[smem, hbm, hbm, hbm, vmem, vmem, hbm, hbm],
            out_specs=(hbm, hbm),
            scratch_shapes=[
                pltpu.VMEM((rows, seq, dim), BF16), pltpu.VMEM((rows, seq, dim), BF16),
                pltpu.VMEM((rows, embed), BF16), pltpu.VMEM((embed, dim), BF16), pltpu.VMEM((embed, dim), BF16),
                pltpu.VMEM((rows, dim), F32), pltpu.VMEM((rows, dim), F32),
                dma((2, CACHE_STEPS)), dma((2, CACHE_STEPS)), dma((3,)),
            ],
            compiler_params=pltpu.CompilerParams(vmem_limit_bytes=24 << 20),
            name="cache_update",
        )(own_lengths, hidden, w_key, w_value, cos, sin, k_cache, v_cache)
        y_packed = pl.pallas_call(
            functools.partial(step_kernel, side),
            out_shape=jax.ShapeDtypeStruct((group, rows // 2, dim), BF16),
            in_specs=[hbm] * 5 + [vmem] * 3,
            out_specs=vmem,
            scratch_shapes=[
                pltpu.VMEM((batch, embed), BF16), pltpu.VMEM(w_query.shape, BF16),
                pltpu.VMEM((side, half, cols), BF16), pltpu.VMEM((group * half, cols), BF16),
                pltpu.VMEM((rows, seq, dim), BF16), pltpu.VMEM((rows, seq, dim), BF16),
                pltpu.VMEM((side, 2 * side, rows // 2, dim), BF16), pltpu.VMEM((group, rows // 2, dim), BF16),
                pltpu.VMEM((rows * heads, dim), F32), pltpu.VMEM((rows // O_STEPS * heads, dim), F32),
                pltpu.VMEM((side, O_STEPS, heads, rows // O_STEPS, dim), BF16),
                pltpu.VMEM((side, 2 * side, rows // 2, dim), BF16), pltpu.VMEM((group, rows // 2, dim), BF16),
                dma((side,)), dma, dma((side,)), dma((O_STEPS,)), dma((O_STEPS,)),
                dma((group,)), dma((group,)), dma((2 * group,)), dma((group,)),
                dma((4 * O_STEPS,)), dma((side, O_STEPS)), dma((group,)), dma((group,)),
            ],
            compiler_params=pltpu.CompilerParams(collective_id=0, has_side_effects=True, vmem_limit_bytes=48 << 20),
            name="attention_step",
        )(hidden, w_query, w_out, k_out, v_out, lens, cos, sin)
        y_local = y_packed.reshape(group, rows // 2, 2, half).transpose(0, 2, 1, 3).reshape(batch, half)
        return y_local, k_out, v_out

    return jax.shard_map(
        local_step,
        mesh=mesh,
        in_specs=(P("dp", None), P(None, "tp"), P(), P(), P("tp", None), cache_spec, cache_spec, P("dp")),
        out_specs=(P("dp", "tp"), cache_spec, cache_spec),
        check_vma=False,
    )
```

```python
import functools
import math

import jax
import jax.numpy as jnp
import numpy as np
from jax import lax
from jax.experimental import pallas as pl
from jax.experimental.pallas import tpu as pltpu
from jax.sharding import PartitionSpec as P

F32, BF16 = jnp.float32, jnp.bfloat16
MESH = pl.DeviceIdType.MESH
O_STEPS = 4
SUB = 8
VMEM_LIMIT = 55 << 20


def step_kernel(side, hidden, wq_turned, w_key, w_value, w_out, k_in, v_in, lengths, freq, y_out, k_buf, v_buf,
                lens, lens_f, h_buf, wq_buf, wk_buf, wv_buf, wo_buf, w_buf, k_new, v_new,
                q_send, q_recv, q_rows, s_rows, p_rows, o_rows, o_buf, y_send, y_recv,
                h_sem, small_sem, wo_sem, k_sem, v_sem,
                q_ssem, q_rsem, w_ssem, w_rsem, w_xsem, o_ssem, o_rsem, y_ssem, y_rsem):
    rows, seq, dim = k_in.shape
    half = dim // 2
    pack = rows // 2
    group = 2 * side * side
    heads = group // 2
    cols = w_buf.shape[1]
    me = lax.axis_index("tp")
    core = lax.rem(me, 2)
    chip = me // 2
    x = lax.rem(chip, side)
    y = chip // side

    def index(xx, yy, cc):
        return (lax.rem(yy, side) * side + lax.rem(xx, side)) * 2 + cc

    def remote(src, dst, ssem, rsem, target):
        return pltpu.make_async_remote_copy(src_ref=src, dst_ref=dst, send_sem=ssem, recv_sem=rsem,
                                            device_id={"tp": target}, device_id_type=MESH)

    def wait_recv(ref, rsem):
        remote(ref, ref, q_ssem, rsem, me).wait_recv()

    def wait_send(ref, ssem):
        remote(ref, ref, ssem, q_rsem, me).wait_send()

    block = rows * 2 * side
    ydest = [lax.rem(y + d, side) for d in (2, 1, 3, 0)]

    def h_part(yy):
        return pl.ds(pl.multiple_of(yy * block, block), block)

    small = [pltpu.make_async_copy(src, dst, small_sem.at[i]) for i, (src, dst) in enumerate(
        ((wq_turned, wq_buf), (lengths, lens), (w_key, wk_buf), (w_value, wv_buf)))]
    h_copies = [pltpu.make_async_copy(hidden.at[h_part(yy)], h_buf.at[h_part(yy)], h_sem.at[i]) for i, yy in enumerate(ydest)]
    wo_copies = [pltpu.make_async_copy(w_out.at[:, pl.ds(i * cols, cols)], wo_buf.at[i], wo_sem.at[i]) for i in range(side)]
    step_rows = rows // O_STEPS
    kv_copies = []
    for k in range(O_STEPS):
        part = pl.ds(k * step_rows, step_rows)
        kv_copies.append((pltpu.make_async_copy(k_in.at[part], k_buf.at[part], k_sem.at[k]),
                          pltpu.make_async_copy(v_in.at[part], v_buf.at[part], v_sem.at[k])))
    small[0].start()
    h_copies[0].start()
    h_copies[1].start()
    small[1].start()

    barrier = pltpu.get_barrier_semaphore()
    peers = [(lax.rem(chip + i, heads)) * 2 + c for i in range(1, heads) for c in range(2)] + [chip * 2 + (1 - core)]
    for peer in peers:
        pl.semaphore_signal(barrier, inc=1, device_id={"tp": peer}, device_id_type=MESH)

    with jax.named_scope("wait_wq"):
        small[0].wait()
    wq = wq_buf[...].T
    own = x * 2 + core
    for i, yy in enumerate(ydest):
        with jax.named_scope("wait_h"):
            h_copies[i].wait()
        if i + 2 < side:
            h_copies[i + 2].start()
        if i == 1:
            for copy in wo_copies + small[2:]:
                copy.start()
        if i == 2:
            for k in range(O_STEPS // 2):
                for copy in kv_copies[k]:
                    copy.start()
        q_val = jnp.dot(h_buf[h_part(yy), :], wq, preferred_element_type=F32).astype(BF16)
        q_val = q_val.reshape(2 * side, 2, pack, half)
        q_send[pl.ds(i * 2 * side, 2 * side)] = jnp.concatenate([q_val[:, 0], q_val[:, 1]], axis=-1)
        if i == 0:
            with jax.named_scope("barrier"):
                pl.semaphore_wait(barrier, len(peers))

        def send_q(j, carry, i=i, yy=yy):
            slot = lax.rem(own + 1 + j, 2 * side)
            remote(q_send.at[i * 2 * side + slot], q_recv.at[me], q_ssem, q_rsem, yy * 2 * side + slot).start()
            return carry

        lax.fori_loop(0, 2 * side if i < side - 1 else 2 * side - 1, send_q, 0)
    q_recv[me] = q_send[(side - 1) * 2 * side + own]
    for k in range(O_STEPS // 2, O_STEPS):
        for copy in kv_copies[k]:
            copy.start()

    def w_slot(t):
        return w_buf.at[pl.ds(pl.multiple_of(t * half, half), half)]

    left, right, other = index(x + side - 1, y, core), index(x + 1, y, core), chip * 2 + (1 - core)
    n_w = [0]

    def send_w(src, t, target):
        n_w[0] += 1
        remote(src, w_slot(t), w_ssem, w_rsem.at[t], target).start()

    def give_w(src, t):
        n_w[0] += 1
        remote(src, w_slot(t), w_ssem, w_xsem, other).start()

    def wait_w(t):
        wait_recv(w_slot(t), w_rsem.at[t])

    with jax.named_scope("send_w"):
        for copy in wo_copies:
            copy.wait()
        for d in (1, 3, 2):
            send_w(wo_buf.at[lax.rem(y + d, side)], me, index(x, y + d, core))
        for target in (right, left):
            send_w(wo_buf.at[y], me, target)
        give_w(wo_buf.at[y], me)
        w_buf[pl.ds(pl.multiple_of(me * half, half), half)] = wo_buf[y]

    def forward_column(d):
        t = index(x, y + d, core)
        wait_w(t)
        for target in (right, left):
            send_w(w_slot(t), t, target)
        give_w(w_slot(t), t)

    def relay_right(d):
        t = index(x + side - 1, y + d, core)
        wait_w(t)
        send_w(w_slot(t), t, right)
        give_w(w_slot(t), t)

    def relay_left(d):
        t = index(x + 1, y + d, core)
        wait_w(t)
        send_w(w_slot(t), t, left)
        give_w(w_slot(t), t)

    def pass_on(xx, d):
        t = index(xx, y + d, core)
        wait_w(t)
        give_w(w_slot(t), t)

    with jax.named_scope("tables"):
        small[1].wait()

        def spread(r, carry):
            lens_f[pl.ds(r, 1), :] = jnp.full((1, dim), lens[me * rows + r].astype(F32))
            return carry

        lax.fori_loop(0, rows, spread, 0, unroll=8)
        angles = lens_f[...] * freq[...]
        cos, sin = jnp.cos(angles), jnp.sin(angles)
        low = lax.broadcasted_iota(jnp.int32, (rows, dim), 1) < half
        low_pack = lax.broadcasted_iota(jnp.int32, (pack, dim), 1) < half
        c_pack = jnp.where(low_pack, cos[:pack], cos[pack:])
        s_pack = jnp.where(low_pack, sin[:pack], sin[pack:])
        small[2].wait()
        small[3].wait()
        h_own = h_buf[pl.ds(pl.multiple_of(me * rows, rows), rows), :]
        key = jnp.dot(h_own, wk_buf[...], preferred_element_type=F32).astype(BF16).astype(F32)
        turned_key = pltpu.roll(key, half, 1)
        k_new[...] = jnp.where(low, key * cos - turned_key * sin, key * cos + turned_key * sin)
        v_new[...] = jnp.dot(h_own, wv_buf[...], preferred_element_type=F32)
    slot_rows = lax.broadcasted_iota(jnp.int32, (seq, dim), 0).astype(F32).astype(BF16)
    with jax.named_scope("patch"):
        for k in range(O_STEPS):
            for copy in kv_copies[k]:
                copy.wait()

            def patch(j, carry, k=k):
                r = k * step_rows + j
                here = slot_rows == lens_f[pl.ds(r, 1), :].astype(BF16)
                k_buf[r] = jnp.where(here, k_new[pl.ds(r, 1), :].astype(BF16), k_buf[r])
                v_buf[r] = jnp.where(here, v_new[pl.ds(r, 1), :].astype(BF16), v_buf[r])
                return carry

            lax.fori_loop(0, step_rows, patch, 0)

    with jax.named_scope("wait_q"):
        wait_recv(q_recv.at[pl.ds(0, group - 1)], q_rsem)
    with jax.named_scope("rope"):
        for i in range(heads):
            p1, p2 = q_recv[2 * i].astype(F32), q_recv[2 * i + 1].astype(F32)
            r1, r2 = p1 * c_pack - p2 * s_pack, p2 * c_pack + p1 * s_pack
            q_rows[pl.ds(i, pack, stride=heads), :] = jnp.where(low_pack, r1, pltpu.roll(r2, half, 1))
            q_rows[pl.ds(pack * heads + i, pack, stride=heads), :] = jnp.where(low_pack, pltpu.roll(r1, half, 1), r2)

    scale = dim ** -0.5
    slots = lax.broadcasted_iota(jnp.int32, (heads, seq), 1).astype(F32)
    up, down = index(x, y + 1, core), index(x, y + side - 1, core)
    y_up, y_down, y_far = lax.rem(y + 1, side), lax.rem(y + side - 1, side), lax.rem(y + 2, side)

    def send_o(yy, k, target):
        piece = o_buf.at[yy * O_STEPS + k]
        remote(piece, piece, o_ssem, o_rsem.at[yy, k], target).start()

    def wait_o(yy, k):
        wait_recv(o_buf.at[yy * O_STEPS + k], o_rsem.at[yy, k])

    def relay_o(k):
        if k % 2 == 0:
            wait_o(y_down, k)
            send_o(y_down, k, up)
        else:
            wait_o(y_up, k)
            send_o(y_up, k, down)

    def score(k, part):
        r = k * step_rows + part
        q_row = q_rows[pl.ds(r * heads, heads), :].astype(BF16)
        scores = lax.dot_general(q_row, k_buf[r], (((1,), (1,)), ((), ())), preferred_element_type=F32) * scale
        last = jnp.concatenate([lens_f[pl.ds(r, 1), :]] * (seq // dim), axis=1)
        s_rows[pl.ds(part * heads, heads), :] = jnp.where(slots <= last, scores, -1e30)

    def attend(k):
        for part in range(step_rows):
            score(k, part)
        for first in range(0, step_rows, SUB):
            span = pl.ds(first * heads, SUB * heads)
            scores = s_rows[span, :]
            weights = jnp.exp(scores - jnp.max(scores, axis=1, keepdims=True))
            p_rows[span, :] = weights.astype(BF16)
            total = jnp.sum(weights, axis=1, keepdims=True)
            for u in range(SUB):
                part = first + u
                summed = jnp.dot(p_rows[pl.ds(part * heads, heads), :], v_buf[k * step_rows + part], preferred_element_type=F32)
                o_rows[pl.ds(part * heads, heads), :] = summed / total[u * heads:(u + 1) * heads]
        for i in range(heads):
            o_buf[y * O_STEPS + k, i] = o_rows[pl.ds(i, step_rows, stride=heads), :].astype(BF16)
        send_o(y, k, up)
        send_o(y, k, down)

    with jax.named_scope("attend0"):
        attend(0)
    with jax.named_scope("column"):
        for d in (1, 3, 2):
            forward_column(d)
    with jax.named_scope("attend1"):
        attend(1)
    with jax.named_scope("relay1"):
        relay_right(0)
        pass_on(x + 1, 0)
    with jax.named_scope("attend2"):
        attend(2)
    with jax.named_scope("relay2"):
        relay_o(0)
    with jax.named_scope("attend3"):
        attend(3)
    with jax.named_scope("relay3"):
        relay_o(1)
        relay_right(1)
        relay_left(3)
        relay_left(2)
    with jax.named_scope("relay4"):
        relay_o(2)
        relay_o(3)
    with jax.named_scope("pass_on"):
        pass_on(x + side - 1, 3)
        pass_on(x + side - 1, 2)
        pass_on(x + 1, 1)
    with jax.named_scope("wait_w_far"):
        for d in (0, 1, 3, 2):
            pass_on(x + 2, d)
    with jax.named_scope("wait_w_other"):
        wait_recv(w_buf.at[pl.ds(0, heads * half)], w_xsem)

    n_y = [0]

    def project(yy):
        n = n_y[0]
        n_y[0] += 1
        lhs = jnp.concatenate([o_buf[pl.ds(yy * O_STEPS, O_STEPS), i].reshape(rows, dim) for i in range(heads)], axis=1)
        res = jnp.dot(lhs, w_buf[...], preferred_element_type=F32)
        row_owner = index(x, yy, core)
        for slot in range(0, 2 * side, 2):
            turned = res[:, slot * half:(slot + 2) * half].T.astype(BF16)
            for c in range(2):
                part = turned[c * half:(c + 1) * half]
                y_send[n * 2 * side + slot + c] = jnp.concatenate([part[:half // 2], part[half // 2:]], axis=1)

        def send_y(j, carry):
            slot = lax.rem(own + 1 + j, 2 * side)
            remote(y_send.at[n * 2 * side + slot], y_recv.at[row_owner], y_ssem, y_rsem, y * 2 * side + slot).start()
            return carry

        lax.fori_loop(0, 2 * side - 1, send_y, 0)
        y_recv[row_owner] = y_send[n * 2 * side + own]

    with jax.named_scope("project0"):
        project(y)
    with jax.named_scope("wait_o_up"):
        wait_o(y_up, 0)
        wait_o(y_up, 2)
    with jax.named_scope("project1"):
        project(y_up)
    with jax.named_scope("wait_o_down"):
        wait_o(y_down, 1)
        wait_o(y_down, 3)
    with jax.named_scope("project2"):
        project(y_down)
    with jax.named_scope("wait_o_far"):
        for k in range(O_STEPS):
            wait_o(y_far, k)
    with jax.named_scope("project3"):
        project(y_far)
    with jax.named_scope("drain"):
        wait_send(q_send.at[pl.ds(0, group - 1)], q_ssem)
        wait_send(w_buf.at[pl.ds(0, n_w[0] * half)], w_ssem)
        wait_send(o_buf.at[pl.ds(0, 3 * O_STEPS)], o_ssem)
    with jax.named_scope("wait_y"):
        wait_recv(y_recv.at[pl.ds(0, side * (2 * side - 1))], y_rsem)
    with jax.named_scope("finish"):
        for i in range(heads):
            a, b = y_recv[2 * i], y_recv[2 * i + 1]
            two_rows = pl.ds(i * 2 * rows, 2 * rows)
            y_out[pl.ds(0, half // 2), two_rows] = jnp.concatenate([a[:, :rows], b[:, :rows]], axis=1)
            y_out[pl.ds(half // 2, half // 2), two_rows] = jnp.concatenate([a[:, rows:], b[:, rows:]], axis=1)
        wait_send(y_send.at[pl.ds(0, side * (2 * side - 1))], y_ssem)


def solution(mesh):
    group = mesh.shape["tp"]
    side = math.isqrt(group // 2)
    cache_spec = P(("dp", "tp"), None, None)
    vmem, hbm = pl.BlockSpec(memory_space=pltpu.VMEM), pl.BlockSpec(memory_space=pltpu.HBM)
    dma = pltpu.SemaphoreType.DMA

    def local_step(hidden, w_query, w_key, w_value, w_out, k_cache, v_cache, lengths):
        rows, seq, dim = k_cache.shape
        batch, embed = hidden.shape
        half = dim // 2
        heads = group * w_query.shape[1] // dim
        cols = w_out.shape[1] // side
        freq = (10000.0 ** (-(np.arange(half) * 2.0) / dim)).astype(np.float32)
        freq = jnp.asarray(np.concatenate([freq, freq])[None, :])
        cache_shape = pltpu.VMEM(k_cache.shape, k_cache.dtype)
        y_turned, k_out, v_out = pl.pallas_call(
            functools.partial(step_kernel, side),
            out_shape=(pltpu.VMEM((w_out.shape[1] // group, batch), BF16), cache_shape, cache_shape),
            in_specs=[hbm] * 8 + [vmem],
            out_specs=(vmem, vmem, vmem),
            scratch_shapes=[
                pltpu.SMEM((batch,), jnp.int32), pltpu.VMEM((rows, dim), F32),
                pltpu.VMEM((batch, embed), BF16), pltpu.VMEM((half, embed), BF16),
                pltpu.VMEM((embed, dim), BF16), pltpu.VMEM((embed, dim), BF16),
                pltpu.VMEM((side, half, cols), BF16), pltpu.VMEM((group * half, cols), BF16),
                pltpu.VMEM((rows, dim), F32), pltpu.VMEM((rows, dim), F32),
                pltpu.VMEM((group, rows // 2, dim), BF16), pltpu.VMEM((group, rows // 2, dim), BF16),
                pltpu.VMEM((rows * heads, dim), F32), pltpu.VMEM((rows // O_STEPS * heads, seq), F32),
                pltpu.VMEM((rows // O_STEPS * heads, seq), BF16), pltpu.VMEM((rows // O_STEPS * heads, dim), F32),
                pltpu.VMEM((side * O_STEPS, heads, rows // O_STEPS, dim), BF16),
                pltpu.VMEM((group, rows // 2, dim), BF16), pltpu.VMEM((group, rows // 2, dim), BF16),
                dma((side,)), dma((4,)), dma((side,)), dma((O_STEPS,)), dma((O_STEPS,)),
                dma, dma, dma, dma((group,)), dma, dma, dma((side, O_STEPS)), dma, dma,
            ],
            compiler_params=pltpu.CompilerParams(collective_id=0, has_side_effects=True, vmem_limit_bytes=VMEM_LIMIT),
            name="attention_step",
        )(hidden, w_query.T, w_key, w_value, w_out, k_cache, v_cache, lengths, freq)
        return y_turned.T, k_out, v_out

    return jax.shard_map(
        local_step,
        mesh=mesh,
        in_specs=(P("dp", None), P(None, "tp"), P(), P(), P("tp", None), cache_spec, cache_spec, P("dp")),
        out_specs=(P("dp", "tp"), cache_spec, cache_spec),
        check_vma=False,
    )
```

```python
import functools
import math

import jax
import jax.numpy as jnp
import numpy as np
from jax import lax
from jax.experimental import pallas as pl
from jax.experimental.pallas import tpu as pltpu
from jax.sharding import PartitionSpec as P

F32, BF16 = jnp.float32, jnp.bfloat16
MESH = pl.DeviceIdType.MESH
O_STEPS = 4
SUB = 8
VMEM_LIMIT = 55 << 20


def step_kernel(side, hidden, wq_turned, w_key, w_value, w_out, k_in, v_in, lengths, freq_in, y_out, k_buf, v_buf,
                lens, freq, lens_f, h_buf, wq_buf, wk_buf, wv_buf, wo_buf, w_buf, k_new, v_new,
                q_send, q_recv, q_rows, s_rows, p_rows, o_rows, o_buf, y_send, y_recv,
                h_sem, small_sem, wo_sem, k_sem, v_sem,
                q_ssem, q_rsem, w_ssem, w_rsem, w_xsem, o_ssem, o_rsem, y_ssem, y_rsem):
    rows, seq, dim = k_in.shape
    half = dim // 2
    pack = rows // 2
    group = 2 * side * side
    heads = group // 2
    cols = w_buf.shape[1]
    me = lax.axis_index("tp")
    core = lax.rem(me, 2)
    chip = me // 2
    x = lax.rem(chip, side)
    y = chip // side

    def index(xx, yy, cc):
        return (lax.rem(yy, side) * side + lax.rem(xx, side)) * 2 + cc

    def remote(src, dst, ssem, rsem, target):
        return pltpu.make_async_remote_copy(src_ref=src, dst_ref=dst, send_sem=ssem, recv_sem=rsem,
                                            device_id={"tp": target}, device_id_type=MESH)

    def wait_recv(ref, rsem):
        remote(ref, ref, q_ssem, rsem, me).wait_recv()

    def wait_send(ref, ssem):
        remote(ref, ref, ssem, q_rsem, me).wait_send()

    block = rows * 2 * side
    ydest = [lax.rem(y + d, side) for d in (2, 1, 3, 0)]

    def h_part(yy):
        return pl.ds(pl.multiple_of(yy * block, block), block)

    small = [pltpu.make_async_copy(src, dst, small_sem.at[i]) for i, (src, dst) in enumerate(
        ((wq_turned, wq_buf), (lengths, lens), (w_key, wk_buf), (w_value, wv_buf), (freq_in, freq)))]
    h_copies = [pltpu.make_async_copy(hidden.at[h_part(yy)], h_buf.at[h_part(yy)], h_sem.at[i]) for i, yy in enumerate(ydest)]
    wo_copies = [pltpu.make_async_copy(w_out.at[:, pl.ds(i * cols, cols)], wo_buf.at[i], wo_sem.at[i]) for i in range(side)]
    step_rows = rows // O_STEPS
    kv_copies = []
    for k in range(O_STEPS):
        part = pl.ds(k * step_rows, step_rows)
        kv_copies.append((pltpu.make_async_copy(k_in.at[part], k_buf.at[part], k_sem.at[k]),
                          pltpu.make_async_copy(v_in.at[part], v_buf.at[part], v_sem.at[k])))
    small[0].start()
    h_copies[0].start()
    for copy in wo_copies:
        copy.start()
    h_copies[1].start()
    small[1].start()
    small[4].start()

    barrier = pltpu.get_barrier_semaphore()
    peers = [(lax.rem(chip + i, heads)) * 2 + c for i in range(1, heads) for c in range(2)] + [chip * 2 + (1 - core)]
    for peer in peers:
        pl.semaphore_signal(barrier, inc=1, device_id={"tp": peer}, device_id_type=MESH)

    def w_slot(t):
        return w_buf.at[pl.ds(pl.multiple_of(t * half, half), half)]

    left, right, other = index(x + side - 1, y, core), index(x + 1, y, core), chip * 2 + (1 - core)
    n_w = [0]

    def send_w(src, t, target):
        n_w[0] += 1
        remote(src, w_slot(t), w_ssem, w_rsem.at[t], target).start()

    def give_w(src, t):
        n_w[0] += 1
        remote(src, w_slot(t), w_ssem, w_xsem, other).start()

    def wait_w(t):
        wait_recv(w_slot(t), w_rsem.at[t])

    def first_w():
        for copy in wo_copies:
            copy.wait()
        for d in (1, 3, 2):
            send_w(wo_buf.at[lax.rem(y + d, side)], me, index(x, y + d, core))

    def own_w():
        for target in (right, left):
            send_w(wo_buf.at[y], me, target)
        give_w(wo_buf.at[y], me)
        w_buf[pl.ds(pl.multiple_of(me * half, half), half)] = wo_buf[y]

    with jax.named_scope("wait_wq"):
        small[0].wait()
    wq = wq_buf[...].T
    own = x * 2 + core
    for i, yy in enumerate(ydest):
        with jax.named_scope("wait_h"):
            h_copies[i].wait()
        if i + 2 < side:
            h_copies[i + 2].start()
        if i == 1:
            for copy in small[2:4]:
                copy.start()
        if i == 2:
            for k in range(O_STEPS // 2):
                for copy in kv_copies[k]:
                    copy.start()
        for part in range(2):
            some = pl.ds(pl.multiple_of(yy * block + part * (block // 2), block // 2), block // 2)
            q_val = jnp.dot(h_buf[some, :], wq, preferred_element_type=F32).astype(BF16)
            q_val = q_val.reshape(side, 2, pack, half)
            q_send[pl.ds(i * 2 * side + part * side, side)] = jnp.concatenate([q_val[:, 0], q_val[:, 1]], axis=-1)
        if i == 0:
            with jax.named_scope("barrier"):
                pl.semaphore_wait(barrier, len(peers))

        def send_q(j, carry, i=i, yy=yy):
            slot = lax.rem(own + 1 + j, 2 * side)
            remote(q_send.at[i * 2 * side + slot], q_recv.at[me], q_ssem, q_rsem, yy * 2 * side + slot).start()
            return carry

        lax.fori_loop(0, 2 * side if i < side - 1 else 2 * side - 1, send_q, 0)
        if i == side - 2:
            first_w()
    own_w()
    q_recv[me] = q_send[(side - 1) * 2 * side + own]
    for k in range(O_STEPS // 2, O_STEPS):
        for copy in kv_copies[k]:
            copy.start()

    def forward_column(d):
        t = index(x, y + d, core)
        wait_w(t)
        for target in (right, left):
            send_w(w_slot(t), t, target)
        give_w(w_slot(t), t)

    def relay_right(d):
        t = index(x + side - 1, y + d, core)
        wait_w(t)
        send_w(w_slot(t), t, right)
        give_w(w_slot(t), t)

    def relay_left(d):
        t = index(x + 1, y + d, core)
        wait_w(t)
        send_w(w_slot(t), t, left)
        give_w(w_slot(t), t)

    def pass_on(xx, d):
        t = index(xx, y + d, core)
        wait_w(t)
        give_w(w_slot(t), t)

    with jax.named_scope("tables"):
        small[1].wait()
        small[4].wait()

        def spread(r, carry):
            lens_f[pl.ds(r, 1), :] = jnp.full((1, dim), lens[me * rows + r].astype(F32))
            return carry

        lax.fori_loop(0, rows, spread, 0, unroll=8)
        angles = lens_f[...] * freq[...]
        cos, sin = jnp.cos(angles), jnp.sin(angles)
        low = lax.broadcasted_iota(jnp.int32, (rows, dim), 1) < half
        low_pack = lax.broadcasted_iota(jnp.int32, (pack, dim), 1) < half
        c_pack = jnp.where(low_pack, cos[:pack], cos[pack:])
        s_pack = jnp.where(low_pack, sin[:pack], sin[pack:])
        small[2].wait()
        small[3].wait()
        h_own = h_buf[pl.ds(pl.multiple_of(me * rows, rows), rows), :]
        key = jnp.dot(h_own, wk_buf[...], preferred_element_type=F32).astype(BF16).astype(F32)
        turned_key = pltpu.roll(key, half, 1)
        k_new[...] = jnp.where(low, key * cos - turned_key * sin, key * cos + turned_key * sin)
        v_new[...] = jnp.dot(h_own, wv_buf[...], preferred_element_type=F32)
    slot_rows = lax.broadcasted_iota(jnp.int32, (seq, dim), 0).astype(F32).astype(BF16)
    with jax.named_scope("patch"):
        for k in range(O_STEPS):
            for copy in kv_copies[k]:
                copy.wait()

            def patch(j, carry, k=k):
                r = k * step_rows + j
                here = slot_rows == lens_f[pl.ds(r, 1), :].astype(BF16)
                k_buf[r] = jnp.where(here, k_new[pl.ds(r, 1), :].astype(BF16), k_buf[r])
                v_buf[r] = jnp.where(here, v_new[pl.ds(r, 1), :].astype(BF16), v_buf[r])
                return carry

            lax.fori_loop(0, step_rows, patch, 0)

    with jax.named_scope("wait_q"):
        wait_recv(q_recv.at[pl.ds(0, group - 1)], q_rsem)
    with jax.named_scope("rope"):
        for i in range(heads):
            p1, p2 = q_recv[2 * i].astype(F32), q_recv[2 * i + 1].astype(F32)
            r1, r2 = p1 * c_pack - p2 * s_pack, p2 * c_pack + p1 * s_pack
            q_rows[pl.ds(i, pack, stride=heads), :] = jnp.where(low_pack, r1, pltpu.roll(r2, half, 1))
            q_rows[pl.ds(pack * heads + i, pack, stride=heads), :] = jnp.where(low_pack, pltpu.roll(r1, half, 1), r2)

    scale = dim ** -0.5
    slots = lax.broadcasted_iota(jnp.int32, (heads, seq), 1).astype(F32)
    up, down = index(x, y + 1, core), index(x, y + side - 1, core)
    y_up, y_down, y_far = lax.rem(y + 1, side), lax.rem(y + side - 1, side), lax.rem(y + 2, side)

    def send_o(yy, k, target):
        piece = o_buf.at[yy * O_STEPS + k]
        remote(piece, piece, o_ssem, o_rsem.at[yy, k], target).start()

    def wait_o(yy, k):
        wait_recv(o_buf.at[yy * O_STEPS + k], o_rsem.at[yy, k])

    def relay_o(k):
        if k % 2 == 0:
            wait_o(y_down, k)
            send_o(y_down, k, up)
        else:
            wait_o(y_up, k)
            send_o(y_up, k, down)

    def score(k, part):
        r = k * step_rows + part
        q_row = q_rows[pl.ds(r * heads, heads), :].astype(BF16)
        scores = lax.dot_general(q_row, k_buf[r], (((1,), (1,)), ((), ())), preferred_element_type=F32) * scale
        last = jnp.concatenate([lens_f[pl.ds(r, 1), :]] * (seq // dim), axis=1)
        s_rows[pl.ds(part * heads, heads), :] = jnp.where(slots <= last, scores, -1e30)

    def attend(k):
        for part in range(step_rows):
            score(k, part)
        for first in range(0, step_rows, SUB):
            span = pl.ds(first * heads, SUB * heads)
            scores = s_rows[span, :]
            weights = jnp.exp(scores - jnp.max(scores, axis=1, keepdims=True))
            p_rows[span, :] = weights.astype(BF16)
            total = jnp.sum(weights, axis=1, keepdims=True)
            for u in range(SUB):
                part = first + u
                summed = jnp.dot(p_rows[pl.ds(part * heads, heads), :], v_buf[k * step_rows + part], preferred_element_type=F32)
                o_rows[pl.ds(part * heads, heads), :] = summed / total[u * heads:(u + 1) * heads]
        for i in range(heads):
            o_buf[y * O_STEPS + k, i] = o_rows[pl.ds(i, step_rows, stride=heads), :].astype(BF16)
        send_o(y, k, up)
        send_o(y, k, down)

    with jax.named_scope("attend0"):
        attend(0)
    with jax.named_scope("column"):
        for d in (1, 3, 2):
            forward_column(d)
    with jax.named_scope("attend1"):
        attend(1)
    with jax.named_scope("relay0"):
        relay_right(0)
        pass_on(x + 1, 0)
    with jax.named_scope("attend2"):
        attend(2)
        attend(3)
    with jax.named_scope("relay1"):
        relay_right(1)
        relay_left(3)
    with jax.named_scope("relay2"):
        relay_o(0)
        relay_left(2)
    with jax.named_scope("relay3"):
        relay_o(1)
        pass_on(x + side - 1, 3)
        pass_on(x + side - 1, 2)
        pass_on(x + 1, 1)
    with jax.named_scope("relay4"):
        relay_o(2)
        relay_o(3)
    with jax.named_scope("wait_w_far"):
        for d in (0, 1, 3, 2):
            pass_on(x + 2, d)
    with jax.named_scope("wait_w_other"):
        wait_recv(w_buf.at[pl.ds(0, heads * half)], w_xsem)

    n_y = [0]

    def project(*sources):
        lhs = [jnp.concatenate([o_buf[pl.ds(yy * O_STEPS, O_STEPS), i].reshape(rows, dim) for i in range(heads)], axis=1)
               for yy in sources]
        res = jnp.dot(jnp.concatenate(lhs, axis=0), w_buf[...], preferred_element_type=F32)
        for m, yy in enumerate(sources):
            n = n_y[0]
            n_y[0] += 1
            row_owner = index(x, yy, core)
            for slot in range(0, 2 * side, 2):
                turned = res[m * rows:(m + 1) * rows, slot * half:(slot + 2) * half].T.astype(BF16)
                for c in range(2):
                    part = turned[c * half:(c + 1) * half]
                    y_send[n * 2 * side + slot + c] = jnp.concatenate([part[:half // 2], part[half // 2:]], axis=1)

            def send_y(j, carry, n=n, row_owner=row_owner):
                slot = lax.rem(own + 1 + j, 2 * side)
                remote(y_send.at[n * 2 * side + slot], y_recv.at[row_owner], y_ssem, y_rsem, y * 2 * side + slot).start()
                return carry

            lax.fori_loop(0, 2 * side - 1, send_y, 0)
            y_recv[row_owner] = y_send[n * 2 * side + own]

    with jax.named_scope("wait_o_near"):
        wait_o(y_up, 0)
        wait_o(y_up, 2)
        wait_o(y_down, 1)
        wait_o(y_down, 3)
    with jax.named_scope("project_near"):
        project(y, y_up, y_down)
    with jax.named_scope("wait_o_far"):
        for k in range(O_STEPS):
            wait_o(y_far, k)
    with jax.named_scope("project_far"):
        project(y_far)
    with jax.named_scope("drain"):
        wait_send(q_send.at[pl.ds(0, group - 1)], q_ssem)
        wait_send(w_buf.at[pl.ds(0, n_w[0] * half)], w_ssem)
        wait_send(o_buf.at[pl.ds(0, 3 * O_STEPS)], o_ssem)
    with jax.named_scope("wait_y"):
        wait_recv(y_recv.at[pl.ds(0, side * (2 * side - 1))], y_rsem)
    with jax.named_scope("finish"):
        for i in range(heads):
            a, b = y_recv[2 * i], y_recv[2 * i + 1]
            two_rows = pl.ds(i * 2 * rows, 2 * rows)
            y_out[pl.ds(0, half // 2), two_rows] = jnp.concatenate([a[:, :rows], b[:, :rows]], axis=1)
            y_out[pl.ds(half // 2, half // 2), two_rows] = jnp.concatenate([a[:, rows:], b[:, rows:]], axis=1)
        wait_send(y_send.at[pl.ds(0, side * (2 * side - 1))], y_ssem)


def write_kernel(y_in, k_in, v_in, y_out, k_out, v_out, sems):
    rows = k_in.shape[0]
    part_rows = rows // O_STEPS
    copies = []
    for src, dst in ((k_in, k_out), (v_in, v_out)):
        for j in range(O_STEPS):
            part = pl.ds(j * part_rows, part_rows)
            copies.append(pltpu.make_async_copy(src.at[part], dst.at[part], sems.at[len(copies)]))
    copies.append(pltpu.make_async_copy(y_in, y_out, sems.at[len(copies)]))
    for copy in copies:
        copy.start()
    for copy in copies:
        copy.wait()


def solution(mesh):
    group = mesh.shape["tp"]
    side = math.isqrt(group // 2)
    cache_spec = P(("dp", "tp"), None, None)
    vmem, hbm = pl.BlockSpec(memory_space=pltpu.VMEM), pl.BlockSpec(memory_space=pltpu.HBM)
    dma = pltpu.SemaphoreType.DMA

    def local_step(hidden, w_query, w_key, w_value, w_out, k_cache, v_cache, lengths):
        rows, seq, dim = k_cache.shape
        batch, embed = hidden.shape
        half = dim // 2
        heads = group * w_query.shape[1] // dim
        cols = w_out.shape[1] // side
        freq = (10000.0 ** (-(np.arange(half) * 2.0) / dim)).astype(np.float32)
        freq = jnp.asarray(np.concatenate([freq, freq])[None, :])
        cache_shape = pltpu.VMEM(k_cache.shape, k_cache.dtype)
        y_shape = ((w_out.shape[1] // group, batch), BF16)
        y_turned, k_new, v_new = pl.pallas_call(
            functools.partial(step_kernel, side),
            out_shape=(pltpu.VMEM(*y_shape), cache_shape, cache_shape),
            in_specs=[hbm] * 9,
            out_specs=(vmem, vmem, vmem),
            scratch_shapes=[
                pltpu.SMEM((batch,), jnp.int32), pltpu.VMEM((1, dim), F32), pltpu.VMEM((rows, dim), F32),
                pltpu.VMEM((batch, embed), BF16), pltpu.VMEM((half, embed), BF16),
                pltpu.VMEM((embed, dim), BF16), pltpu.VMEM((embed, dim), BF16),
                pltpu.VMEM((side, half, cols), BF16), pltpu.VMEM((group * half, cols), BF16),
                pltpu.VMEM((rows, dim), F32), pltpu.VMEM((rows, dim), F32),
                pltpu.VMEM((group, rows // 2, dim), BF16), pltpu.VMEM((group, rows // 2, dim), BF16),
                pltpu.VMEM((rows * heads, dim), F32), pltpu.VMEM((rows // O_STEPS * heads, seq), F32),
                pltpu.VMEM((rows // O_STEPS * heads, seq), BF16), pltpu.VMEM((rows // O_STEPS * heads, dim), F32),
                pltpu.VMEM((side * O_STEPS, heads, rows // O_STEPS, dim), BF16),
                pltpu.VMEM((group, rows // 2, dim), BF16), pltpu.VMEM((group, rows // 2, dim), BF16),
                dma((side,)), dma((5,)), dma((side,)), dma((O_STEPS,)), dma((O_STEPS,)),
                dma, dma, dma, dma((group,)), dma, dma, dma((side, O_STEPS)), dma, dma,
            ],
            compiler_params=pltpu.CompilerParams(collective_id=0, has_side_effects=True, vmem_limit_bytes=VMEM_LIMIT),
            name="attention_step",
        )(hidden, w_query.T, w_key, w_value, w_out, k_cache, v_cache, lengths, freq)
        whole = jax.ShapeDtypeStruct(k_cache.shape, k_cache.dtype)
        y_turned, k_out, v_out = pl.pallas_call(
            write_kernel,
            out_shape=(jax.ShapeDtypeStruct(*y_shape), whole, whole),
            in_specs=[vmem] * 3,
            out_specs=(hbm, hbm, hbm),
            scratch_shapes=[dma((2 * O_STEPS + 1,))],
            compiler_params=pltpu.CompilerParams(vmem_limit_bytes=1 << 20),
            name="write_results",
        )(y_turned, k_new, v_new)
        return y_turned.T, k_out, v_out

    return jax.shard_map(
        local_step,
        mesh=mesh,
        in_specs=(P("dp", None), P(None, "tp"), P(), P(), P("tp", None), cache_spec, cache_spec, P("dp")),
        out_specs=(P("dp", "tp"), cache_spec, cache_spec),
        check_vma=False,
    )
```

```python
import functools
import math

import jax
import jax.numpy as jnp
import numpy as np
from jax import lax
from jax.experimental import pallas as pl
from jax.experimental.pallas import tpu as pltpu
from jax.sharding import PartitionSpec as P

F32, BF16 = jnp.float32, jnp.bfloat16
MESH = pl.DeviceIdType.MESH
O_STEPS = 4
SUB = 8
VMEM_LIMIT = 55 << 20
FIRST_W = 0


def step_kernel(side, hidden, wq_turned, w_key, w_value, w_out, k_in, v_in, lengths, freq_in, y_out, k_buf, v_buf,
                lens, freq, lens_f, h_buf, wq_buf, wk_buf, wv_buf, wo_buf, w_buf, k_new, v_new,
                q_send, q_recv, q_rows, s_rows, p_rows, o_rows, o_buf, y_acc, y_send, y_recv,
                h_sem, small_sem, wo_sem, k_sem, v_sem,
                q_ssem, q_rsem, w_ssem, w_rsem, w_xsem, o_ssem, o_rsem, near_ssem, far_ssem, near_rsem, far_rsem):
    rows, seq, dim = k_in.shape
    half = dim // 2
    pack = rows // 2
    group = 2 * side * side
    heads = group // 2
    cols = w_buf.shape[1]
    me = lax.axis_index("tp")
    core = lax.rem(me, 2)
    chip = me // 2
    x = lax.rem(chip, side)
    y = chip // side

    def index(xx, yy, cc):
        return (lax.rem(yy, side) * side + lax.rem(xx, side)) * 2 + cc

    def remote(src, dst, ssem, rsem, target):
        return pltpu.make_async_remote_copy(src_ref=src, dst_ref=dst, send_sem=ssem, recv_sem=rsem,
                                            device_id={"tp": target}, device_id_type=MESH)

    def wait_recv(ref, rsem):
        remote(ref, ref, q_ssem, rsem, me).wait_recv()

    def wait_send(ref, ssem):
        remote(ref, ref, ssem, q_rsem, me).wait_send()

    block = rows * 2 * side
    ydest = [lax.rem(y + d, side) for d in (2, 1, 3, 0)]

    def h_part(yy):
        return pl.ds(pl.multiple_of(yy * block, block), block)

    small = [pltpu.make_async_copy(src, dst, small_sem.at[i]) for i, (src, dst) in enumerate(
        ((wq_turned, wq_buf), (lengths, lens), (w_key, wk_buf), (w_value, wv_buf), (freq_in, freq)))]
    h_copies = [pltpu.make_async_copy(hidden.at[h_part(yy)], h_buf.at[h_part(yy)], h_sem.at[i]) for i, yy in enumerate(ydest)]
    wo_copies = [pltpu.make_async_copy(w_out.at[:, pl.ds(i * cols, cols)], wo_buf.at[i], wo_sem.at[i]) for i in range(side)]
    step_rows = rows // O_STEPS
    kv_copies = []
    for k in range(O_STEPS):
        part = pl.ds(k * step_rows, step_rows)
        kv_copies.append((pltpu.make_async_copy(k_in.at[part], k_buf.at[part], k_sem.at[k]),
                          pltpu.make_async_copy(v_in.at[part], v_buf.at[part], v_sem.at[k])))
    small[0].start()
    h_copies[0].start()
    for copy in wo_copies:
        copy.start()
    h_copies[1].start()
    small[1].start()
    small[4].start()

    barrier = pltpu.get_barrier_semaphore()
    peers = [(lax.rem(chip + i, heads)) * 2 + c for i in range(1, heads) for c in range(2)] + [chip * 2 + (1 - core)]
    for peer in peers:
        pl.semaphore_signal(barrier, inc=1, device_id={"tp": peer}, device_id_type=MESH)

    def w_row(t):
        return (lax.rem(t, 2) * heads + t // 2) * half

    def w_slot(t):
        return w_buf.at[pl.ds(pl.multiple_of(w_row(t), half), half)]

    left, right, other = index(x + side - 1, y, core), index(x + 1, y, core), chip * 2 + (1 - core)
    n_w = [0]

    def send_w(src, t, target):
        n_w[0] += 1
        remote(src, w_slot(t), w_ssem, w_rsem.at[t], target).start()

    def give_w(src, t):
        n_w[0] += 1
        remote(src, w_slot(t), w_ssem, w_xsem, other).start()

    def wait_w(t):
        wait_recv(w_slot(t), w_rsem.at[t])

    def first_w():
        for copy in wo_copies:
            copy.wait()
        for d in (1, 3, 2):
            send_w(wo_buf.at[lax.rem(y + d, side)], me, index(x, y + d, core))

    def own_w():
        for target in (right, left):
            send_w(wo_buf.at[y], me, target)
        give_w(wo_buf.at[y], me)
        w_buf[pl.ds(pl.multiple_of(w_row(me), half), half)] = wo_buf[y]

    with jax.named_scope("wait_wq"):
        small[0].wait()
    wq = wq_buf[...].T
    own = x * 2 + core
    for i, yy in enumerate(ydest):
        with jax.named_scope("wait_h"):
            h_copies[i].wait()
        if i + 2 < side:
            h_copies[i + 2].start()
        if i == 1:
            for copy in small[2:4]:
                copy.start()
        if i == 2:
            for k in range(O_STEPS // 2):
                for copy in kv_copies[k]:
                    copy.start()
        for part in range(2):
            some = pl.ds(pl.multiple_of(yy * block + part * (block // 2), block // 2), block // 2)
            q_val = jnp.dot(h_buf[some, :], wq, preferred_element_type=F32).astype(BF16)
            q_val = q_val.reshape(side, 2, pack, half)
            q_send[pl.ds(i * 2 * side + part * side, side)] = jnp.concatenate([q_val[:, 0], q_val[:, 1]], axis=-1)
        if i == 0:
            with jax.named_scope("barrier"):
                pl.semaphore_wait(barrier, len(peers))

        for j in range(2 * side if i < side - 1 else 2 * side - 1):
            slot = lax.rem(own + 1 + j, 2 * side)
            remote(q_send.at[i * 2 * side + slot], q_recv.at[me], q_ssem, q_rsem, yy * 2 * side + slot).start()
        if i == FIRST_W:
            first_w()
    own_w()
    q_recv[me] = q_send[(side - 1) * 2 * side + own]
    for k in range(O_STEPS // 2, O_STEPS):
        for copy in kv_copies[k]:
            copy.start()

    def forward_column(d):
        t = index(x, y + d, core)
        wait_w(t)
        for target in (right, left):
            send_w(w_slot(t), t, target)
        give_w(w_slot(t), t)

    def relay_right(d):
        t = index(x + side - 1, y + d, core)
        wait_w(t)
        send_w(w_slot(t), t, right)
        give_w(w_slot(t), t)

    def relay_left(d):
        t = index(x + 1, y + d, core)
        wait_w(t)
        send_w(w_slot(t), t, left)
        give_w(w_slot(t), t)

    def pass_on(xx, d):
        t = index(xx, y + d, core)
        wait_w(t)
        give_w(w_slot(t), t)

    with jax.named_scope("tables"):
        small[1].wait()
        small[4].wait()

        def spread(r, carry):
            lens_f[pl.ds(r, 1), :] = jnp.full((1, dim), lens[me * rows + r].astype(F32))
            return carry

        lax.fori_loop(0, rows, spread, 0, unroll=8)
        angles = lens_f[...] * freq[...]
        cos, sin = jnp.cos(angles), jnp.sin(angles)
        low = lax.broadcasted_iota(jnp.int32, (rows, dim), 1) < half
        low_pack = lax.broadcasted_iota(jnp.int32, (pack, dim), 1) < half
        c_pack = jnp.where(low_pack, cos[:pack], cos[pack:])
        s_pack = jnp.where(low_pack, sin[:pack], sin[pack:])
        small[2].wait()
        small[3].wait()
        h_own = h_buf[pl.ds(pl.multiple_of(me * rows, rows), rows), :]
        key = jnp.dot(h_own, wk_buf[...], preferred_element_type=F32).astype(BF16).astype(F32)
        turned_key = pltpu.roll(key, half, 1)
        k_new[...] = jnp.where(low, key * cos - turned_key * sin, key * cos + turned_key * sin)
        v_new[...] = jnp.dot(h_own, wv_buf[...], preferred_element_type=F32)
    slot_rows = lax.broadcasted_iota(jnp.int32, (seq, dim), 0).astype(F32).astype(BF16)
    with jax.named_scope("patch"):
        for k in range(O_STEPS):
            for copy in kv_copies[k]:
                copy.wait()

            def patch(j, carry, k=k):
                r = k * step_rows + j
                here = slot_rows == lens_f[pl.ds(r, 1), :].astype(BF16)
                k_buf[r] = jnp.where(here, k_new[pl.ds(r, 1), :].astype(BF16), k_buf[r])
                v_buf[r] = jnp.where(here, v_new[pl.ds(r, 1), :].astype(BF16), v_buf[r])
                return carry

            lax.fori_loop(0, step_rows, patch, 0)

    with jax.named_scope("column"):
        for d in (1, 3, 2):
            forward_column(d)

    with jax.named_scope("wait_q"):
        wait_recv(q_recv.at[pl.ds(0, group - 1)], q_rsem)
    with jax.named_scope("rope"):
        for i in range(heads):
            p1, p2 = q_recv[2 * i].astype(F32), q_recv[2 * i + 1].astype(F32)
            r1, r2 = p1 * c_pack - p2 * s_pack, p2 * c_pack + p1 * s_pack
            q_rows[pl.ds(i, pack, stride=heads), :] = jnp.where(low_pack, r1, pltpu.roll(r2, half, 1))
            q_rows[pl.ds(pack * heads + i, pack, stride=heads), :] = jnp.where(low_pack, pltpu.roll(r1, half, 1), r2)

    scale = dim ** -0.5
    slots = lax.broadcasted_iota(jnp.int32, (heads, seq), 1).astype(F32)
    up, down = index(x, y + 1, core), index(x, y + side - 1, core)
    y_up, y_down, y_far = lax.rem(y + 1, side), lax.rem(y + side - 1, side), lax.rem(y + 2, side)

    def send_o(yy, k, target):
        piece = o_buf.at[yy * O_STEPS + k]
        remote(piece, piece, o_ssem, o_rsem.at[yy, k], target).start()

    def wait_o(yy, k):
        wait_recv(o_buf.at[yy * O_STEPS + k], o_rsem.at[yy, k])

    def relay_o(k):
        if k % 2 == 0:
            wait_o(y_down, k)
            send_o(y_down, k, up)
        else:
            wait_o(y_up, k)
            send_o(y_up, k, down)

    def score(k, part):
        r = k * step_rows + part
        q_row = q_rows[pl.ds(r * heads, heads), :].astype(BF16)
        scores = lax.dot_general(q_row, k_buf[r], (((1,), (1,)), ((), ())), preferred_element_type=F32) * scale
        last = jnp.concatenate([lens_f[pl.ds(r, 1), :]] * (seq // dim), axis=1)
        s_rows[pl.ds(part * heads, heads), :] = jnp.where(slots <= last, scores, -1e30)

    low_step = lax.broadcasted_iota(jnp.int32, (step_rows, dim), 1) < half

    def attend(k):
        for part in range(step_rows):
            score(k, part)
        for first in range(0, step_rows, SUB):
            span = pl.ds(first * heads, SUB * heads)
            scores = s_rows[span, :]
            weights = jnp.exp(scores - jnp.max(scores, axis=1, keepdims=True))
            p_rows[span, :] = weights.astype(BF16)
            total = jnp.sum(weights, axis=1, keepdims=True)
            for u in range(SUB):
                part = first + u
                summed = jnp.dot(p_rows[pl.ds(part * heads, heads), :], v_buf[k * step_rows + part], preferred_element_type=F32)
                o_rows[pl.ds(part * heads, heads), :] = summed / total[u * heads:(u + 1) * heads]
        for i in range(heads // 2):
            even, odd = (o_rows[pl.ds(2 * i + j, step_rows, stride=heads), :] for j in range(2))
            o_buf[y * O_STEPS + k, i] = jnp.where(low_step, even, pltpu.roll(odd, half, 1)).astype(BF16)
            o_buf[y * O_STEPS + k, heads // 2 + i] = jnp.where(low_step, pltpu.roll(even, half, 1), odd).astype(BF16)
        send_o(y, k, up)
        send_o(y, k, down)

    with jax.named_scope("attend0"):
        attend(0)
    with jax.named_scope("relay0"):
        relay_right(0)
        pass_on(x + 1, 0)
    with jax.named_scope("attend1"):
        attend(1)
    with jax.named_scope("relay1"):
        relay_right(1)
    with jax.named_scope("attend2"):
        attend(2)
        attend(3)
    with jax.named_scope("relay2"):
        relay_left(3)
        relay_left(2)
    with jax.named_scope("relay3"):
        relay_o(0)
        pass_on(x + side - 1, 3)
        pass_on(x + side - 1, 2)
        pass_on(x + 1, 1)
    with jax.named_scope("relay4"):
        relay_o(1)
        relay_o(2)
    with jax.named_scope("relay5"):
        relay_o(3)
    with jax.named_scope("wait_w_far"):
        for d in (0, 1, 3, 2):
            pass_on(x + 2, d)
    sources = [y, y_up, y_down, y_far]
    near = side - 1
    depth = heads * half

    def partial(some, c):
        lhs = [jnp.concatenate([o_buf[pl.ds(sources[n] * O_STEPS, O_STEPS), c * (heads // 2) + i].reshape(rows, dim)
                                for i in range(heads // 2)], axis=1) for n in some]
        return jnp.dot(jnp.concatenate(lhs, axis=0), w_buf[pl.ds(pl.multiple_of(c * depth, depth), depth), :],
                       preferred_element_type=F32)

    def place(some, res):
        for m, n in enumerate(some):
            for slot in range(0, 2 * side, 2):
                turned = res[m * rows:(m + 1) * rows, slot * half:(slot + 2) * half].T.astype(BF16)
                for c in range(2):
                    part = turned[c * half:(c + 1) * half]
                    y_send[slot + c, n] = jnp.concatenate([part[:half // 2], part[half // 2:]], axis=1)

    with jax.named_scope("wait_o_near"):
        wait_o(y_up, 0)
        wait_o(y_up, 2)
        wait_o(y_down, 1)
        wait_o(y_down, 3)
    with jax.named_scope("near_own"):
        y_acc[...] = partial(range(near), core)
    with jax.named_scope("wait_w_other"):
        wait_recv(w_buf.at[pl.ds(0, depth)], w_xsem)
    with jax.named_scope("near_other"):
        place(range(near), y_acc[...] + partial(range(near), 1 - core))
        for j in range(1, 2 * side):
            slot = lax.rem(own + j, 2 * side)
            remote(y_send.at[slot, pl.ds(0, near)], y_recv.at[own, pl.ds(0, near)], near_ssem, near_rsem, y * 2 * side + slot).start()
    with jax.named_scope("wait_o_far"):
        for k in range(O_STEPS):
            wait_o(y_far, k)
    with jax.named_scope("project_far"):
        place([near], partial([near], core) + partial([near], 1 - core))
        for j in range(1, 2 * side):
            slot = lax.rem(own + j, 2 * side)
            remote(y_send.at[slot, near], y_recv.at[own, near], far_ssem, far_rsem, y * 2 * side + slot).start()
        y_recv[own] = y_send[own]

    def finish(n):
        for i in range(side):
            a, b = y_recv[2 * i, n], y_recv[2 * i + 1, n]
            span = pl.ds(pl.multiple_of((sources[n] * side + i) * 2 * rows, 2 * rows), 2 * rows)
            y_out[pl.ds(0, half // 2), span] = jnp.concatenate([a[:, :rows], b[:, :rows]], axis=1)
            y_out[pl.ds(half // 2, half // 2), span] = jnp.concatenate([a[:, rows:], b[:, rows:]], axis=1)

    others = pl.ds(0, 2 * side - 1)
    with jax.named_scope("drain"):
        wait_send(q_send.at[pl.ds(0, group - 1)], q_ssem)
        wait_send(w_buf.at[pl.ds(0, n_w[0] * half)], w_ssem)
        wait_send(o_buf.at[pl.ds(0, 3 * O_STEPS)], o_ssem)
        wait_send(y_send.at[others, pl.ds(0, near)], near_ssem)
    with jax.named_scope("wait_y_near"):
        wait_recv(y_recv.at[others, pl.ds(0, near)], near_rsem)
    for n in range(near):
        finish(n)
    with jax.named_scope("wait_y_far"):
        wait_recv(y_recv.at[others, near], far_rsem)
    finish(near)
    wait_send(y_send.at[others, near], far_ssem)


def write_kernel(y_in, k_in, v_in, y_out, k_out, v_out, sems):
    rows = k_in.shape[0]
    part_rows = rows // O_STEPS
    copies = []
    for src, dst in ((k_in, k_out), (v_in, v_out)):
        for j in range(O_STEPS):
            part = pl.ds(j * part_rows, part_rows)
            copies.append(pltpu.make_async_copy(src.at[part], dst.at[part], sems.at[len(copies)]))
    copies.append(pltpu.make_async_copy(y_in, y_out, sems.at[len(copies)]))
    for copy in copies:
        copy.start()
    for copy in copies:
        copy.wait()


def solution(mesh):
    group = mesh.shape["tp"]
    side = math.isqrt(group // 2)
    cache_spec = P(("dp", "tp"), None, None)
    vmem, hbm = pl.BlockSpec(memory_space=pltpu.VMEM), pl.BlockSpec(memory_space=pltpu.HBM)
    dma = pltpu.SemaphoreType.DMA

    def local_step(hidden, w_query, w_key, w_value, w_out, k_cache, v_cache, lengths):
        rows, seq, dim = k_cache.shape
        batch, embed = hidden.shape
        half = dim // 2
        heads = group * w_query.shape[1] // dim
        cols = w_out.shape[1] // side
        freq = (10000.0 ** (-(np.arange(half) * 2.0) / dim)).astype(np.float32)
        freq = jnp.asarray(np.concatenate([freq, freq])[None, :])
        cache_shape = pltpu.VMEM(k_cache.shape, k_cache.dtype)
        packed = pltpu.VMEM((2 * side, side, half // 2, dim), BF16)
        y_shape = ((w_out.shape[1] // group, batch), BF16)
        y_turned, k_new, v_new = pl.pallas_call(
            functools.partial(step_kernel, side),
            out_shape=(pltpu.VMEM(*y_shape), cache_shape, cache_shape),
            in_specs=[hbm] * 9,
            out_specs=(vmem, vmem, vmem),
            scratch_shapes=[
                pltpu.SMEM((batch,), jnp.int32), pltpu.VMEM((1, dim), F32), pltpu.VMEM((rows, dim), F32),
                pltpu.VMEM((batch, embed), BF16), pltpu.VMEM((half, embed), BF16),
                pltpu.VMEM((embed, dim), BF16), pltpu.VMEM((embed, dim), BF16),
                pltpu.VMEM((side, half, cols), BF16), pltpu.VMEM((group * half, cols), BF16),
                pltpu.VMEM((rows, dim), F32), pltpu.VMEM((rows, dim), F32),
                pltpu.VMEM((group, rows // 2, dim), BF16), pltpu.VMEM((group, rows // 2, dim), BF16),
                pltpu.VMEM((rows * heads, dim), F32), pltpu.VMEM((rows // O_STEPS * heads, seq), F32),
                pltpu.VMEM((rows // O_STEPS * heads, seq), BF16), pltpu.VMEM((rows // O_STEPS * heads, dim), F32),
                pltpu.VMEM((side * O_STEPS, heads, rows // O_STEPS, dim), BF16),
                pltpu.VMEM(((side - 1) * rows, cols), F32), packed, packed,
                dma((side,)), dma((5,)), dma((side,)), dma((O_STEPS,)), dma((O_STEPS,)),
                dma, dma, dma, dma((group,)), dma, dma, dma((side, O_STEPS)), dma, dma, dma, dma,
            ],
            compiler_params=pltpu.CompilerParams(collective_id=0, has_side_effects=True, vmem_limit_bytes=VMEM_LIMIT),
            name="attention_step",
        )(hidden, w_query.T, w_key, w_value, w_out, k_cache, v_cache, lengths, freq)
        whole = jax.ShapeDtypeStruct(k_cache.shape, k_cache.dtype)
        y_turned, k_out, v_out = pl.pallas_call(
            write_kernel,
            out_shape=(jax.ShapeDtypeStruct(*y_shape), whole, whole),
            in_specs=[vmem] * 3,
            out_specs=(hbm, hbm, hbm),
            scratch_shapes=[dma((2 * O_STEPS + 1,))],
            compiler_params=pltpu.CompilerParams(vmem_limit_bytes=1 << 20),
            name="write_results",
        )(y_turned, k_new, v_new)
        return y_turned.T, k_out, v_out

    return jax.shard_map(
        local_step,
        mesh=mesh,
        in_specs=(P("dp", None), P(None, "tp"), P(), P(), P("tp", None), cache_spec, cache_spec, P("dp")),
        out_specs=(P("dp", "tp"), cache_spec, cache_spec),
        check_vma=False,
    )
```

```python
import functools
import math

import jax
import jax.numpy as jnp
import numpy as np
from jax import lax
from jax.experimental import pallas as pl
from jax.experimental.pallas import tpu as pltpu
from jax.sharding import PartitionSpec as P

F32, BF16 = jnp.float32, jnp.bfloat16
MESH = pl.DeviceIdType.MESH
O_STEPS = 4
SUB = 8
VMEM_LIMIT = 55 << 20
FIRST_W = 0


def step_kernel(side, hidden, wq_turned, w_key, w_value, w_out, k_in, v_in, lengths, freq_in, y_out, k_buf, v_buf,
                lens, freq, lens_f, h_buf, wq_buf, wk_buf, wv_buf, wo_buf, w_buf, k_new, v_new,
                q_send, q_recv, q_rows, s_rows, p_rows, o_rows, o_buf, y_acc, y_send, y_recv,
                h_sem, small_sem, wo_sem, k_sem, v_sem,
                q_ssem, q_rsem, q_rsem_late, w_ssem, w_rsem, w_xsem, o_ssem, o_rsem, near_ssem, far_ssem, near_rsem, far_rsem):
    rows, seq, dim = k_in.shape
    half = dim // 2
    pack = rows // 2
    group = 2 * side * side
    heads = group // 2
    cols = w_buf.shape[1]
    me = lax.axis_index("tp")
    core = lax.rem(me, 2)
    chip = me // 2
    x = lax.rem(chip, side)
    y = chip // side

    def index(xx, yy, cc):
        return (lax.rem(yy, side) * side + lax.rem(xx, side)) * 2 + cc

    def remote(src, dst, ssem, rsem, target):
        return pltpu.make_async_remote_copy(src_ref=src, dst_ref=dst, send_sem=ssem, recv_sem=rsem,
                                            device_id={"tp": target}, device_id_type=MESH)

    def wait_recv(ref, rsem):
        remote(ref, ref, q_ssem, rsem, me).wait_recv()

    def wait_send(ref, ssem):
        remote(ref, ref, ssem, q_rsem, me).wait_send()

    block = rows * 2 * side
    ydest = [lax.rem(y + d, side) for d in (2, 1, 3, 0)]

    def h_part(yy):
        return pl.ds(pl.multiple_of(yy * block, block), block)

    small = [pltpu.make_async_copy(src, dst, small_sem.at[i]) for i, (src, dst) in enumerate(
        ((wq_turned, wq_buf), (lengths, lens), (w_key, wk_buf), (w_value, wv_buf), (freq_in, freq)))]
    h_copies = [pltpu.make_async_copy(hidden.at[h_part(yy)], h_buf.at[h_part(yy)], h_sem.at[i]) for i, yy in enumerate(ydest)]
    wo_copies = [pltpu.make_async_copy(w_out.at[:, pl.ds(i * cols, cols)], wo_buf.at[i], wo_sem.at[i]) for i in range(side)]
    step_rows = rows // O_STEPS
    kv_copies = []
    for k in range(O_STEPS):
        part = pl.ds(k * step_rows, step_rows)
        kv_copies.append((pltpu.make_async_copy(k_in.at[part], k_buf.at[part], k_sem.at[k]),
                          pltpu.make_async_copy(v_in.at[part], v_buf.at[part], v_sem.at[k])))
    order = (0, 2, 1, 3)
    small[0].start()
    h_copies[0].start()

    barrier = pltpu.get_barrier_semaphore()
    peers = [(lax.rem(chip + i, heads)) * 2 + c for i in range(1, heads) for c in range(2)] + [chip * 2 + (1 - core)]
    for peer in peers:
        pl.semaphore_signal(barrier, inc=1, device_id={"tp": peer}, device_id_type=MESH)
    for copy in wo_copies + [h_copies[1], small[1], small[4]]:
        copy.start()

    def w_row(t):
        return (lax.rem(t, 2) * heads + t // 2) * half

    def w_slot(t):
        return w_buf.at[pl.ds(pl.multiple_of(w_row(t), half), half)]

    left, right, other = index(x + side - 1, y, core), index(x + 1, y, core), chip * 2 + (1 - core)
    n_w = [0]

    def send_w(src, t, target):
        n_w[0] += 1
        remote(src, w_slot(t), w_ssem, w_rsem.at[t], target).start()

    def give_w(src, t):
        n_w[0] += 1
        remote(src, w_slot(t), w_ssem, w_xsem, other).start()

    def wait_w(t):
        wait_recv(w_slot(t), w_rsem.at[t])

    def first_w():
        for copy in wo_copies:
            copy.wait()
        for d in (1, 3, 2):
            send_w(wo_buf.at[lax.rem(y + d, side)], me, index(x, y + d, core))

    def own_w():
        for target in (right, left):
            send_w(wo_buf.at[y], me, target)
        give_w(wo_buf.at[y], me)
        w_buf[pl.ds(pl.multiple_of(w_row(me), half), half)] = wo_buf[y]

    with jax.named_scope("wait_wq"):
        small[0].wait()
    wq = wq_buf[...].T
    own = x * 2 + core
    quarter = pack // 2

    def send_q(i, part, rsem):
        some = pl.ds(part * quarter, quarter)
        for j in range(2 * side if i < side - 1 else 2 * side - 1):
            slot = lax.rem(own + 1 + j, 2 * side)
            remote(q_send.at[i * 2 * side + slot, some], q_recv.at[me, some], q_ssem, rsem, ydest[i] * 2 * side + slot).start()

    for i, yy in enumerate(ydest):
        with jax.named_scope("wait_h"):
            h_copies[i].wait()
        if i + 2 < side:
            h_copies[i + 2].start()
        if i == 1:
            for copy in small[2:4]:
                copy.start()
        if i == 2:
            for k in order[:2]:
                for copy in kv_copies[k]:
                    copy.start()
        for part in range(2):
            some = pl.ds(pl.multiple_of(yy * block + part * (block // 2), block // 2), block // 2)
            q_val = jnp.dot(h_buf[some, :], wq, preferred_element_type=F32).astype(BF16)
            q_val = q_val.reshape(side, 2, pack, half)
            q_send[pl.ds(i * 2 * side + part * side, side)] = jnp.concatenate([q_val[:, 0], q_val[:, 1]], axis=-1)
        if i == 0:
            with jax.named_scope("barrier"):
                pl.semaphore_wait(barrier, len(peers))

        send_q(i, 0, q_rsem)
        if i == FIRST_W:
            first_w()
    own_w()
    for i in range(side):
        send_q(i, 1, q_rsem_late)
    q_recv[me] = q_send[(side - 1) * 2 * side + own]
    for k in order[2:]:
        for copy in kv_copies[k]:
            copy.start()

    def forward_column(d):
        t = index(x, y + d, core)
        wait_w(t)
        for target in (right, left):
            send_w(w_slot(t), t, target)
        give_w(w_slot(t), t)

    def relay_right(d):
        t = index(x + side - 1, y + d, core)
        wait_w(t)
        send_w(w_slot(t), t, right)
        give_w(w_slot(t), t)

    def relay_left(d):
        t = index(x + 1, y + d, core)
        wait_w(t)
        send_w(w_slot(t), t, left)
        give_w(w_slot(t), t)

    def pass_on(xx, d):
        t = index(xx, y + d, core)
        wait_w(t)
        give_w(w_slot(t), t)

    with jax.named_scope("tables"):
        small[1].wait()
        small[4].wait()

        def spread(r, carry):
            lens_f[pl.ds(r, 1), :] = jnp.full((1, dim), lens[me * rows + r].astype(F32))
            return carry

        lax.fori_loop(0, rows, spread, 0, unroll=8)
        angles = lens_f[...] * freq[...]
        cos, sin = jnp.cos(angles), jnp.sin(angles)
        low = lax.broadcasted_iota(jnp.int32, (rows, dim), 1) < half
        low_pack = lax.broadcasted_iota(jnp.int32, (pack, dim), 1) < half
        c_pack = jnp.where(low_pack, cos[:pack], cos[pack:])
        s_pack = jnp.where(low_pack, sin[:pack], sin[pack:])
        small[2].wait()
        small[3].wait()
        h_own = h_buf[pl.ds(pl.multiple_of(me * rows, rows), rows), :]
        key = jnp.dot(h_own, wk_buf[...], preferred_element_type=F32).astype(BF16).astype(F32)
        turned_key = pltpu.roll(key, half, 1)
        k_new[...] = jnp.where(low, key * cos - turned_key * sin, key * cos + turned_key * sin)
        v_new[...] = jnp.dot(h_own, wv_buf[...], preferred_element_type=F32)
    slot_rows = lax.broadcasted_iota(jnp.int32, (seq, dim), 0).astype(F32).astype(BF16)

    def patch(k):
        for copy in kv_copies[k]:
            copy.wait()

        def patch_row(j, carry):
            r = k * step_rows + j
            here = slot_rows == lens_f[pl.ds(r, 1), :].astype(BF16)
            k_buf[r] = jnp.where(here, k_new[pl.ds(r, 1), :].astype(BF16), k_buf[r])
            v_buf[r] = jnp.where(here, v_new[pl.ds(r, 1), :].astype(BF16), v_buf[r])
            return carry

        lax.fori_loop(0, step_rows, patch_row, 0)

    with jax.named_scope("patch"):
        for k in order:
            patch(k)
    with jax.named_scope("column"):
        for d in (1, 3, 2):
            forward_column(d)

    def wait_q(part, rsem):
        wait_recv(q_recv.at[pl.ds(0, group - 1), pl.ds(part * quarter, quarter)], rsem)

    low_quarter = lax.broadcasted_iota(jnp.int32, (quarter, dim), 1) < half

    def rope(part):
        span = pl.ds(part * quarter, quarter)
        c_part, s_part = c_pack[part * quarter:(part + 1) * quarter], s_pack[part * quarter:(part + 1) * quarter]
        for i in range(heads):
            p1, p2 = q_recv[2 * i, span, :].astype(F32), q_recv[2 * i + 1, span, :].astype(F32)
            r1, r2 = p1 * c_part - p2 * s_part, p2 * c_part + p1 * s_part
            at = part * quarter * heads + i
            q_rows[pl.ds(at, quarter, stride=heads), :] = jnp.where(low_quarter, r1, pltpu.roll(r2, half, 1))
            q_rows[pl.ds(pack * heads + at, quarter, stride=heads), :] = jnp.where(low_quarter, pltpu.roll(r1, half, 1), r2)

    scale = dim ** -0.5
    slots = lax.broadcasted_iota(jnp.int32, (heads, seq), 1).astype(F32)
    up, down = index(x, y + 1, core), index(x, y + side - 1, core)
    y_up, y_down, y_far = lax.rem(y + 1, side), lax.rem(y + side - 1, side), lax.rem(y + 2, side)

    def send_o(yy, k, target, some=slice(None)):
        piece = o_buf.at[yy * O_STEPS + k, some]
        remote(piece, piece, o_ssem, o_rsem.at[yy, k], target).start()

    def wait_o(yy, k):
        wait_recv(o_buf.at[yy * O_STEPS + k], o_rsem.at[yy, k])

    def relay_o(k):
        wait_o(y_down, k)
        send_o(y_down, k, up, pl.ds(0, heads // 2))
        wait_o(y_up, k)
        send_o(y_up, k, down, pl.ds(heads // 2, heads // 2))

    def score(k, part):
        r = k * step_rows + part
        q_row = q_rows[pl.ds(r * heads, heads), :].astype(BF16)
        scores = lax.dot_general(q_row, k_buf[r], (((1,), (1,)), ((), ())), preferred_element_type=F32) * scale
        last = jnp.concatenate([lens_f[pl.ds(r, 1), :]] * (seq // dim), axis=1)
        s_rows[pl.ds(part * heads, heads), :] = jnp.where(slots <= last, scores, -1e30)

    low_step = lax.broadcasted_iota(jnp.int32, (step_rows, dim), 1) < half

    def attend(k):
        for part in range(step_rows):
            score(k, part)
        for first in range(0, step_rows, SUB):
            span = pl.ds(first * heads, SUB * heads)
            scores = s_rows[span, :]
            weights = jnp.exp(scores - jnp.max(scores, axis=1, keepdims=True))
            p_rows[span, :] = weights.astype(BF16)
            total = jnp.sum(weights, axis=1, keepdims=True)
            for u in range(SUB):
                part = first + u
                summed = jnp.dot(p_rows[pl.ds(part * heads, heads), :], v_buf[k * step_rows + part], preferred_element_type=F32)
                o_rows[pl.ds(part * heads, heads), :] = summed / total[u * heads:(u + 1) * heads]
        for i in range(heads // 2):
            even, odd = (o_rows[pl.ds(2 * i + j, step_rows, stride=heads), :] for j in range(2))
            o_buf[y * O_STEPS + k, i] = jnp.where(low_step, even, pltpu.roll(odd, half, 1)).astype(BF16)
            o_buf[y * O_STEPS + k, heads // 2 + i] = jnp.where(low_step, pltpu.roll(even, half, 1), odd).astype(BF16)
        send_o(y, k, up)
        send_o(y, k, down)

    with jax.named_scope("wait_q"):
        wait_q(0, q_rsem)
    with jax.named_scope("attend0"):
        rope(0)
        attend(0)
    with jax.named_scope("relay0"):
        relay_right(0)
        pass_on(x + 1, 0)
    with jax.named_scope("attend1"):
        attend(2)
    with jax.named_scope("wait_q_late"):
        wait_q(1, q_rsem_late)
    with jax.named_scope("attend2"):
        rope(1)
        attend(1)
        attend(3)
    with jax.named_scope("relay2"):
        relay_right(1)
        relay_left(3)
        relay_left(2)
    with jax.named_scope("relay3"):
        relay_o(0)
        pass_on(x + side - 1, 3)
        pass_on(x + side - 1, 2)
        pass_on(x + 1, 1)
    with jax.named_scope("relay4"):
        relay_o(2)
        relay_o(1)
    with jax.named_scope("wait_w_far"):
        for d in (0, 1, 3, 2):
            pass_on(x + 2, d)
    with jax.named_scope("relay5"):
        relay_o(3)
    sources = [y, y_up, y_down, y_far]
    near = side - 1
    depth = heads * half

    def partial(some, c):
        lhs = [jnp.concatenate([o_buf[pl.ds(sources[n] * O_STEPS, O_STEPS), c * (heads // 2) + i].reshape(rows, dim)
                                for i in range(heads // 2)], axis=1) for n in some]
        return jnp.dot(jnp.concatenate(lhs, axis=0), w_buf[pl.ds(pl.multiple_of(c * depth, depth), depth), :],
                       preferred_element_type=F32)

    def place(some, res):
        for m, n in enumerate(some):
            for slot in range(0, 2 * side, 2):
                turned = res[m * rows:(m + 1) * rows, slot * half:(slot + 2) * half].T.astype(BF16)
                for c in range(2):
                    part = turned[c * half:(c + 1) * half]
                    y_send[slot + c, n] = jnp.concatenate([part[:half // 2], part[half // 2:]], axis=1)

    with jax.named_scope("near_own"):
        y_acc[...] = partial(range(near), core)
    with jax.named_scope("wait_w_other"):
        wait_recv(w_buf.at[pl.ds(0, depth)], w_xsem)
    with jax.named_scope("near_other"):
        place(range(near), y_acc[...] + partial(range(near), 1 - core))
        for j in range(1, 2 * side):
            slot = lax.rem(own + j, 2 * side)
            remote(y_send.at[slot, pl.ds(0, near)], y_recv.at[own, pl.ds(0, near)], near_ssem, near_rsem, y * 2 * side + slot).start()
    with jax.named_scope("wait_o_far"):
        for k in range(O_STEPS):
            wait_o(y_far, k)
    with jax.named_scope("project_far"):
        place([near], partial([near], core) + partial([near], 1 - core))
        for j in range(1, 2 * side):
            slot = lax.rem(own + j, 2 * side)
            remote(y_send.at[slot, near], y_recv.at[own, near], far_ssem, far_rsem, y * 2 * side + slot).start()
        y_recv[own] = y_send[own]

    def finish(n):
        for i in range(side):
            a, b = y_recv[2 * i, n], y_recv[2 * i + 1, n]
            span = pl.ds(pl.multiple_of((sources[n] * side + i) * 2 * rows, 2 * rows), 2 * rows)
            y_out[pl.ds(0, half // 2), span] = jnp.concatenate([a[:, :rows], b[:, :rows]], axis=1)
            y_out[pl.ds(half // 2, half // 2), span] = jnp.concatenate([a[:, rows:], b[:, rows:]], axis=1)

    others = pl.ds(0, 2 * side - 1)
    with jax.named_scope("drain"):
        wait_send(q_send.at[pl.ds(0, group - 1)], q_ssem)
        wait_send(w_buf.at[pl.ds(0, n_w[0] * half)], w_ssem)
        wait_send(o_buf.at[pl.ds(0, 3 * O_STEPS)], o_ssem)
        wait_send(y_send.at[others, pl.ds(0, near)], near_ssem)
    with jax.named_scope("wait_y_near"):
        wait_recv(y_recv.at[others, pl.ds(0, near)], near_rsem)
    for n in range(near):
        finish(n)
    with jax.named_scope("wait_y_far"):
        wait_recv(y_recv.at[others, near], far_rsem)
    finish(near)
    wait_send(y_send.at[others, near], far_ssem)


def write_kernel(y_in, k_in, v_in, y_out, k_out, v_out, sems):
    rows = k_in.shape[0]
    part_rows = rows // O_STEPS
    copies = []
    for src, dst in ((k_in, k_out), (v_in, v_out)):
        for j in range(O_STEPS):
            part = pl.ds(j * part_rows, part_rows)
            copies.append(pltpu.make_async_copy(src.at[part], dst.at[part], sems.at[len(copies)]))
    copies.append(pltpu.make_async_copy(y_in, y_out, sems.at[len(copies)]))
    for copy in copies:
        copy.start()
    for copy in copies:
        copy.wait()


def solution(mesh):
    group = mesh.shape["tp"]
    side = math.isqrt(group // 2)
    cache_spec = P(("dp", "tp"), None, None)
    vmem, hbm = pl.BlockSpec(memory_space=pltpu.VMEM), pl.BlockSpec(memory_space=pltpu.HBM)
    dma = pltpu.SemaphoreType.DMA

    def local_step(hidden, w_query, w_key, w_value, w_out, k_cache, v_cache, lengths):
        rows, seq, dim = k_cache.shape
        batch, embed = hidden.shape
        half = dim // 2
        heads = group * w_query.shape[1] // dim
        cols = w_out.shape[1] // side
        freq = (10000.0 ** (-(np.arange(half) * 2.0) / dim)).astype(np.float32)
        freq = jnp.asarray(np.concatenate([freq, freq])[None, :])
        cache_shape = pltpu.VMEM(k_cache.shape, k_cache.dtype)
        packed = pltpu.VMEM((2 * side, side, half // 2, dim), BF16)
        y_shape = ((w_out.shape[1] // group, batch), BF16)
        y_turned, k_new, v_new = pl.pallas_call(
            functools.partial(step_kernel, side),
            out_shape=(pltpu.VMEM(*y_shape), cache_shape, cache_shape),
            in_specs=[hbm] * 9,
            out_specs=(vmem, vmem, vmem),
            scratch_shapes=[
                pltpu.SMEM((batch,), jnp.int32), pltpu.VMEM((1, dim), F32), pltpu.VMEM((rows, dim), F32),
                pltpu.VMEM((batch, embed), BF16), pltpu.VMEM((half, embed), BF16),
                pltpu.VMEM((embed, dim), BF16), pltpu.VMEM((embed, dim), BF16),
                pltpu.VMEM((side, half, cols), BF16), pltpu.VMEM((group * half, cols), BF16),
                pltpu.VMEM((rows, dim), F32), pltpu.VMEM((rows, dim), F32),
                pltpu.VMEM((group, rows // 2, dim), BF16), pltpu.VMEM((group, rows // 2, dim), BF16),
                pltpu.VMEM((rows * heads, dim), F32), pltpu.VMEM((rows // O_STEPS * heads, seq), F32),
                pltpu.VMEM((rows // O_STEPS * heads, seq), BF16), pltpu.VMEM((rows // O_STEPS * heads, dim), F32),
                pltpu.VMEM((side * O_STEPS, heads, rows // O_STEPS, dim), BF16),
                pltpu.VMEM(((side - 1) * rows, cols), F32), packed, packed,
                dma((side,)), dma((5,)), dma((side,)), dma((O_STEPS,)), dma((O_STEPS,)),
                dma, dma, dma, dma, dma((group,)), dma, dma, dma((side, O_STEPS)), dma, dma, dma, dma,
            ],
            compiler_params=pltpu.CompilerParams(collective_id=0, has_side_effects=True, vmem_limit_bytes=VMEM_LIMIT),
            name="attention_step",
        )(hidden, w_query.T, w_key, w_value, w_out, k_cache, v_cache, lengths, freq)
        whole = jax.ShapeDtypeStruct(k_cache.shape, k_cache.dtype)
        y_turned, k_out, v_out = pl.pallas_call(
            write_kernel,
            out_shape=(jax.ShapeDtypeStruct(*y_shape), whole, whole),
            in_specs=[vmem] * 3,
            out_specs=(hbm, hbm, hbm),
            scratch_shapes=[dma((2 * O_STEPS + 1,))],
            compiler_params=pltpu.CompilerParams(vmem_limit_bytes=1 << 20),
            name="write_results",
        )(y_turned, k_new, v_new)
        return y_turned.T, k_out, v_out

    return jax.shard_map(
        local_step,
        mesh=mesh,
        in_specs=(P("dp", None), P(None, "tp"), P(), P(), P("tp", None), cache_spec, cache_spec, P("dp")),
        out_specs=(P("dp", "tp"), cache_spec, cache_spec),
        check_vma=False,
    )
```

```python
import functools
import math

import jax
import jax.numpy as jnp
import numpy as np
from jax import lax
from jax.experimental import pallas as pl
from jax.experimental.pallas import tpu as pltpu
from jax.sharding import PartitionSpec as P

F32, BF16 = jnp.float32, jnp.bfloat16
MESH = pl.DeviceIdType.MESH
O_STEPS = 4
WRITES = 1
SUB = 8
VMEM_LIMIT = 55 << 20
FIRST_W = 0


def step_kernel(side, hidden, wq_turned, w_key, w_value, w_out, k_in, v_in, lengths, freq_in, y_out, k_buf, v_buf,
                lens, freq, lens_f, h_buf, wq_buf, wk_buf, wv_buf, wo_buf, w_buf, k_new, v_new,
                q_send, q_recv, q_rows, s_rows, p_rows, o_rows, o_buf, y_acc, y_send, y_recv,
                h_sem, small_sem, wo_sem, k_sem, v_sem,
                q_ssem, q_rsem, q_rsem_late, w_ssem, w_rsem, w_xsem, o_ssem, o_rsem, near_ssem, far_ssem, near_rsem, far_rsem):
    rows, seq, dim = k_in.shape
    half = dim // 2
    pack = rows // 2
    group = 2 * side * side
    heads = group // 2
    cols = w_buf.shape[1]
    me = lax.axis_index("tp")
    core = lax.rem(me, 2)
    chip = me // 2
    x = lax.rem(chip, side)
    y = chip // side

    def index(xx, yy, cc):
        return (lax.rem(yy, side) * side + lax.rem(xx, side)) * 2 + cc

    def remote(src, dst, ssem, rsem, target):
        return pltpu.make_async_remote_copy(src_ref=src, dst_ref=dst, send_sem=ssem, recv_sem=rsem,
                                            device_id={"tp": target}, device_id_type=MESH)

    def wait_recv(ref, rsem):
        remote(ref, ref, q_ssem, rsem, me).wait_recv()

    def wait_send(ref, ssem):
        remote(ref, ref, ssem, q_rsem, me).wait_send()

    block = rows * 2 * side
    ydest = [lax.rem(y + d, side) for d in (2, 1, 3, 0)]

    def h_part(yy):
        return pl.ds(pl.multiple_of(yy * block, block), block)

    small = [pltpu.make_async_copy(src, dst, small_sem.at[i]) for i, (src, dst) in enumerate(
        ((wq_turned, wq_buf), (lengths, lens), (w_key, wk_buf), (w_value, wv_buf), (freq_in, freq)))]
    h_copies = [pltpu.make_async_copy(hidden.at[h_part(yy)], h_buf.at[h_part(yy)], h_sem.at[i]) for i, yy in enumerate(ydest)]
    wo_copies = [pltpu.make_async_copy(w_out.at[:, pl.ds(i * cols, cols)], wo_buf.at[i], wo_sem.at[i]) for i in range(side)]
    step_rows = rows // O_STEPS
    kv_copies = []
    for k in range(O_STEPS):
        part = pl.ds(k * step_rows, step_rows)
        kv_copies.append((pltpu.make_async_copy(k_in.at[part], k_buf.at[part], k_sem.at[k]),
                          pltpu.make_async_copy(v_in.at[part], v_buf.at[part], v_sem.at[k])))
    order = (0, 2, 1, 3)
    small[0].start()
    h_copies[0].start()

    barrier = pltpu.get_barrier_semaphore()
    peers = [(lax.rem(chip + i, heads)) * 2 + c for i in range(1, heads) for c in range(2)] + [chip * 2 + (1 - core)]
    for peer in peers:
        pl.semaphore_signal(barrier, inc=1, device_id={"tp": peer}, device_id_type=MESH)
    for copy in wo_copies + [h_copies[1], small[1], small[4]]:
        copy.start()

    def w_row(t):
        return (lax.rem(t, 2) * heads + t // 2) * half

    def w_slot(t):
        return w_buf.at[pl.ds(pl.multiple_of(w_row(t), half), half)]

    left, right, other = index(x + side - 1, y, core), index(x + 1, y, core), chip * 2 + (1 - core)
    n_w = [0]

    def send_w(src, t, target, first=0, size=None):
        size = half if size is None else size
        some = pl.ds(first, size)
        n_w[0] += size
        remote(src.at[some], w_slot(t).at[some], w_ssem, w_rsem.at[t], target).start()

    def give_w(src, t):
        n_w[0] += half
        remote(src, w_slot(t), w_ssem, w_xsem, other).start()

    def wait_w(t):
        wait_recv(w_slot(t), w_rsem.at[t])

    def first_w():
        for copy in wo_copies:
            copy.wait()
        for d in (1, 3, 2):
            send_w(wo_buf.at[lax.rem(y + d, side)], me, index(x, y + d, core))

    def own_w():
        for target in (right, left):
            send_w(wo_buf.at[y], me, target)
        give_w(wo_buf.at[y], me)
        w_buf[pl.ds(pl.multiple_of(w_row(me), half), half)] = wo_buf[y]

    with jax.named_scope("wait_wq"):
        small[0].wait()
    wq = wq_buf[...].T
    own = x * 2 + core
    quarter = pack // 2

    def send_q(i, part, rsem):
        some = pl.ds(part * quarter, quarter)
        slots = [lax.rem(x + d, side) * 2 + c for d in (2, 1, 3) for c in range(2)] + [x * 2 + 1 - core]
        for slot in slots + ([own] if i < side - 1 else []):
            remote(q_send.at[i * 2 * side + slot, some], q_recv.at[me, some], q_ssem, rsem, ydest[i] * 2 * side + slot).start()

    for i, yy in enumerate(ydest):
        with jax.named_scope("wait_h"):
            h_copies[i].wait()
        if i + 2 < side:
            h_copies[i + 2].start()
        if i == 1:
            for copy in small[2:4]:
                copy.start()
        if i == 2:
            for k in order[:2]:
                for copy in kv_copies[k]:
                    copy.start()
        for part in range(2):
            some = pl.ds(pl.multiple_of(yy * block + part * (block // 2), block // 2), block // 2)
            q_val = jnp.dot(h_buf[some, :], wq, preferred_element_type=F32).astype(BF16)
            q_val = q_val.reshape(side, 2, pack, half)
            q_send[pl.ds(i * 2 * side + part * side, side)] = jnp.concatenate([q_val[:, 0], q_val[:, 1]], axis=-1)
        if i == 0:
            with jax.named_scope("barrier"):
                pl.semaphore_wait(barrier, len(peers))

        send_q(i, 0, q_rsem)
        if i == FIRST_W:
            first_w()
    own_w()
    for i in range(side):
        send_q(i, 1, q_rsem_late)
    q_recv[me] = q_send[(side - 1) * 2 * side + own]
    for k in order[2:]:
        for copy in kv_copies[k]:
            copy.start()

    def forward_column(d):
        t = index(x, y + d, core)
        wait_w(t)
        for target in (left, right):
            send_w(w_slot(t), t, target)
        give_w(w_slot(t), t)

    def relay_right(d):
        t = index(x + side - 1, y + d, core)
        wait_w(t)
        send_w(w_slot(t), t, right)
        give_w(w_slot(t), t)

    def relay_both(d):
        for xx, target, first in ((x + side - 1, right, 0), (x + 1, left, half // 2)):
            t = index(xx, y + d, core)
            wait_w(t)
            send_w(w_slot(t), t, target, first, half // 2)
            give_w(w_slot(t), t)

    def relay_left(d):
        t = index(x + 1, y + d, core)
        wait_w(t)
        send_w(w_slot(t), t, left)
        give_w(w_slot(t), t)

    def pass_on(xx, d):
        t = index(xx, y + d, core)
        wait_w(t)
        give_w(w_slot(t), t)

    with jax.named_scope("tables"):
        small[1].wait()
        small[4].wait()

        def spread(r, carry):
            lens_f[pl.ds(r, 1), :] = jnp.full((1, dim), lens[me * rows + r].astype(F32))
            return carry

        lax.fori_loop(0, rows, spread, 0, unroll=8)
        angles = lens_f[...] * freq[...]
        cos, sin = jnp.cos(angles), jnp.sin(angles)
        low = lax.broadcasted_iota(jnp.int32, (rows, dim), 1) < half
        low_pack = lax.broadcasted_iota(jnp.int32, (pack, dim), 1) < half
        c_pack = jnp.where(low_pack, cos[:pack], cos[pack:])
        s_pack = jnp.where(low_pack, sin[:pack], sin[pack:])
        small[2].wait()
        small[3].wait()
        h_own = h_buf[pl.ds(pl.multiple_of(me * rows, rows), rows), :]
        key = jnp.dot(h_own, wk_buf[...], preferred_element_type=F32).astype(BF16).astype(F32)
        turned_key = pltpu.roll(key, half, 1)
        k_new[...] = jnp.where(low, key * cos - turned_key * sin, key * cos + turned_key * sin)
        v_new[...] = jnp.dot(h_own, wv_buf[...], preferred_element_type=F32)
    slot_rows = lax.broadcasted_iota(jnp.int32, (seq, dim), 0).astype(F32).astype(BF16)

    def patch(k):
        for copy in kv_copies[k]:
            copy.wait()

        def patch_row(j, carry):
            r = k * step_rows + j
            here = slot_rows == lens_f[pl.ds(r, 1), :].astype(BF16)
            k_buf[r] = jnp.where(here, k_new[pl.ds(r, 1), :].astype(BF16), k_buf[r])
            v_buf[r] = jnp.where(here, v_new[pl.ds(r, 1), :].astype(BF16), v_buf[r])
            return carry

        lax.fori_loop(0, step_rows, patch_row, 0)

    with jax.named_scope("patch"):
        for k in order:
            patch(k)
    with jax.named_scope("column"):
        for d in (1, 3, 2):
            forward_column(d)

    def wait_q(part, rsem):
        wait_recv(q_recv.at[pl.ds(0, group - 1), pl.ds(part * quarter, quarter)], rsem)

    low_quarter = lax.broadcasted_iota(jnp.int32, (quarter, dim), 1) < half

    def rope(part):
        span = pl.ds(part * quarter, quarter)
        c_part, s_part = c_pack[part * quarter:(part + 1) * quarter], s_pack[part * quarter:(part + 1) * quarter]
        for i in range(heads):
            p1, p2 = q_recv[2 * i, span, :].astype(F32), q_recv[2 * i + 1, span, :].astype(F32)
            r1, r2 = p1 * c_part - p2 * s_part, p2 * c_part + p1 * s_part
            at = part * quarter * heads + i
            q_rows[pl.ds(at, quarter, stride=heads), :] = jnp.where(low_quarter, r1, pltpu.roll(r2, half, 1))
            q_rows[pl.ds(pack * heads + at, quarter, stride=heads), :] = jnp.where(low_quarter, pltpu.roll(r1, half, 1), r2)

    scale = dim ** -0.5
    slots = lax.broadcasted_iota(jnp.int32, (heads, seq), 1).astype(F32)
    up, down = index(x, y + 1, core), index(x, y + side - 1, core)
    y_up, y_down, y_far = lax.rem(y + 1, side), lax.rem(y + side - 1, side), lax.rem(y + 2, side)

    def send_o(yy, k, target, some=slice(None)):
        piece = o_buf.at[yy * O_STEPS + k, some]
        remote(piece, piece, o_ssem, o_rsem.at[yy, k], target).start()

    def wait_o(yy, k):
        wait_recv(o_buf.at[yy * O_STEPS + k], o_rsem.at[yy, k])

    def relay_o(k):
        wait_o(y_down, k)
        send_o(y_down, k, up, pl.ds(0, heads // 2))
        wait_o(y_up, k)
        send_o(y_up, k, down, pl.ds(heads // 2, heads // 2))

    def score(k, part):
        r = k * step_rows + part
        q_row = q_rows[pl.ds(r * heads, heads), :].astype(BF16)
        scores = lax.dot_general(q_row, k_buf[r], (((1,), (1,)), ((), ())), preferred_element_type=F32) * scale
        last = jnp.concatenate([lens_f[pl.ds(r, 1), :]] * (seq // dim), axis=1)
        s_rows[pl.ds(part * heads, heads), :] = jnp.where(slots <= last, scores, -1e30)

    low_step = lax.broadcasted_iota(jnp.int32, (step_rows, dim), 1) < half

    def attend(k):
        for part in range(step_rows):
            score(k, part)
        for first in range(0, step_rows, SUB):
            span = pl.ds(first * heads, SUB * heads)
            scores = s_rows[span, :]
            weights = jnp.exp(scores - jnp.max(scores, axis=1, keepdims=True))
            p_rows[span, :] = weights.astype(BF16)
            total = jnp.sum(weights, axis=1, keepdims=True)
            for u in range(SUB):
                part = first + u
                summed = jnp.dot(p_rows[pl.ds(part * heads, heads), :], v_buf[k * step_rows + part], preferred_element_type=F32)
                o_rows[pl.ds(part * heads, heads), :] = summed / total[u * heads:(u + 1) * heads]
        for i in range(heads // 2):
            even, odd = (o_rows[pl.ds(2 * i + j, step_rows, stride=heads), :] for j in range(2))
            o_buf[y * O_STEPS + k, i] = jnp.where(low_step, even, pltpu.roll(odd, half, 1)).astype(BF16)
            o_buf[y * O_STEPS + k, heads // 2 + i] = jnp.where(low_step, pltpu.roll(even, half, 1), odd).astype(BF16)
        send_o(y, k, up)
        send_o(y, k, down)

    with jax.named_scope("wait_q"):
        wait_q(0, q_rsem)
    with jax.named_scope("attend0"):
        rope(0)
        attend(0)
    with jax.named_scope("relay0"):
        relay_right(0)
        pass_on(x + 1, 0)
    with jax.named_scope("attend1"):
        attend(2)
    with jax.named_scope("wait_q_late"):
        wait_q(1, q_rsem_late)
    with jax.named_scope("attend2"):
        rope(1)
        attend(1)
        attend(3)
    with jax.named_scope("relay2"):
        relay_right(1)
        relay_left(3)
        relay_both(2)
    with jax.named_scope("relay3"):
        relay_o(0)
        pass_on(x + side - 1, 3)
        pass_on(x + 1, 1)
    with jax.named_scope("relay4"):
        relay_o(2)
        relay_o(1)
    with jax.named_scope("relay5"):
        relay_o(3)
    with jax.named_scope("wait_w_far"):
        for d in (0, 1, 3, 2):
            pass_on(x + 2, d)
    sources = [y, y_up, y_down, y_far]
    near = side - 1
    depth = heads * half

    def row_peers():
        return [lax.rem(x + d, side) * 2 + c for d in (2, 1, 3) for c in range(2)] + [x * 2 + 1 - core]

    def partial(some, c):
        lhs = [jnp.concatenate([o_buf[pl.ds(sources[n] * O_STEPS, O_STEPS), c * (heads // 2) + i].reshape(rows, dim)
                                for i in range(heads // 2)], axis=1) for n in some]
        return jnp.dot(jnp.concatenate(lhs, axis=0), w_buf[pl.ds(pl.multiple_of(c * depth, depth), depth), :],
                       preferred_element_type=F32)

    def place(some, res):
        for m, n in enumerate(some):
            for slot in range(0, 2 * side, 2):
                turned = res[m * rows:(m + 1) * rows, slot * half:(slot + 2) * half].T.astype(BF16)
                for c in range(2):
                    part = turned[c * half:(c + 1) * half]
                    y_send[slot + c, n] = jnp.concatenate([part[:half // 2], part[half // 2:]], axis=1)

    with jax.named_scope("near_own"):
        y_acc[...] = partial(range(near), core)
    with jax.named_scope("wait_w_other"):
        wait_recv(w_buf.at[pl.ds(0, depth)], w_xsem)
    with jax.named_scope("near_other"):
        place(range(near), y_acc[...] + partial(range(near), 1 - core))
        for slot in row_peers():
            remote(y_send.at[slot, pl.ds(0, near)], y_recv.at[own, pl.ds(0, near)], near_ssem, near_rsem, y * 2 * side + slot).start()
    with jax.named_scope("wait_o_far"):
        for k in range(O_STEPS):
            wait_o(y_far, k)
    with jax.named_scope("project_far"):
        place([near], partial([near], core) + partial([near], 1 - core))
        for slot in row_peers():
            remote(y_send.at[slot, near], y_recv.at[own, near], far_ssem, far_rsem, y * 2 * side + slot).start()
        y_recv[own] = y_send[own]

    def finish(n):
        for i in range(side):
            a, b = y_recv[2 * i, n], y_recv[2 * i + 1, n]
            span = pl.ds(pl.multiple_of((sources[n] * side + i) * 2 * rows, 2 * rows), 2 * rows)
            y_out[pl.ds(0, half // 2), span] = jnp.concatenate([a[:, :rows], b[:, :rows]], axis=1)
            y_out[pl.ds(half // 2, half // 2), span] = jnp.concatenate([a[:, rows:], b[:, rows:]], axis=1)

    others = pl.ds(0, 2 * side - 1)
    with jax.named_scope("drain"):
        wait_send(q_send.at[pl.ds(0, group - 1)], q_ssem)
        wait_send(w_buf.at[pl.ds(0, n_w[0])], w_ssem)
        wait_send(o_buf.at[pl.ds(0, 3 * O_STEPS)], o_ssem)
        wait_send(y_send.at[others, pl.ds(0, near)], near_ssem)
    with jax.named_scope("wait_y_near"):
        wait_recv(y_recv.at[others, pl.ds(0, near)], near_rsem)
    for n in range(near):
        finish(n)
    with jax.named_scope("wait_y_far"):
        wait_recv(y_recv.at[others, near], far_rsem)
    finish(near)
    wait_send(y_send.at[others, near], far_ssem)


def write_kernel(y_in, k_in, v_in, y_out, k_out, v_out, sems):
    rows = k_in.shape[0]
    part_rows = rows // WRITES
    copies = []
    for src, dst in ((k_in, k_out), (v_in, v_out)):
        for j in range(WRITES):
            part = pl.ds(j * part_rows, part_rows)
            copies.append(pltpu.make_async_copy(src.at[part], dst.at[part], sems.at[len(copies)]))
    copies.append(pltpu.make_async_copy(y_in, y_out, sems.at[len(copies)]))
    for copy in copies:
        copy.start()
    for copy in copies:
        copy.wait()


def solution(mesh):
    group = mesh.shape["tp"]
    side = math.isqrt(group // 2)
    cache_spec = P(("dp", "tp"), None, None)
    vmem, hbm = pl.BlockSpec(memory_space=pltpu.VMEM), pl.BlockSpec(memory_space=pltpu.HBM)
    dma = pltpu.SemaphoreType.DMA

    def local_step(hidden, w_query, w_key, w_value, w_out, k_cache, v_cache, lengths):
        rows, seq, dim = k_cache.shape
        batch, embed = hidden.shape
        half = dim // 2
        heads = group * w_query.shape[1] // dim
        cols = w_out.shape[1] // side
        freq = (10000.0 ** (-(np.arange(half) * 2.0) / dim)).astype(np.float32)
        freq = jnp.asarray(np.concatenate([freq, freq])[None, :])
        cache_shape = pltpu.VMEM(k_cache.shape, k_cache.dtype)
        packed = pltpu.VMEM((2 * side, side, half // 2, dim), BF16)
        y_shape = ((w_out.shape[1] // group, batch), BF16)
        y_turned, k_new, v_new = pl.pallas_call(
            functools.partial(step_kernel, side),
            out_shape=(pltpu.VMEM(*y_shape), cache_shape, cache_shape),
            in_specs=[hbm] * 9,
            out_specs=(vmem, vmem, vmem),
            scratch_shapes=[
                pltpu.SMEM((batch,), jnp.int32), pltpu.VMEM((1, dim), F32), pltpu.VMEM((rows, dim), F32),
                pltpu.VMEM((batch, embed), BF16), pltpu.VMEM((half, embed), BF16),
                pltpu.VMEM((embed, dim), BF16), pltpu.VMEM((embed, dim), BF16),
                pltpu.VMEM((side, half, cols), BF16), pltpu.VMEM((group * half, cols), BF16),
                pltpu.VMEM((rows, dim), F32), pltpu.VMEM((rows, dim), F32),
                pltpu.VMEM((group, rows // 2, dim), BF16), pltpu.VMEM((group, rows // 2, dim), BF16),
                pltpu.VMEM((rows * heads, dim), F32), pltpu.VMEM((rows // O_STEPS * heads, seq), F32),
                pltpu.VMEM((rows // O_STEPS * heads, seq), BF16), pltpu.VMEM((rows // O_STEPS * heads, dim), F32),
                pltpu.VMEM((side * O_STEPS, heads, rows // O_STEPS, dim), BF16),
                pltpu.VMEM(((side - 1) * rows, cols), F32), packed, packed,
                dma((side,)), dma((5,)), dma((side,)), dma((O_STEPS,)), dma((O_STEPS,)),
                dma, dma, dma, dma, dma((group,)), dma, dma, dma((side, O_STEPS)), dma, dma, dma, dma,
            ],
            compiler_params=pltpu.CompilerParams(collective_id=0, has_side_effects=True, vmem_limit_bytes=VMEM_LIMIT),
            name="attention_step",
        )(hidden, w_query.T, w_key, w_value, w_out, k_cache, v_cache, lengths, freq)
        whole = jax.ShapeDtypeStruct(k_cache.shape, k_cache.dtype)
        y_turned, k_out, v_out = pl.pallas_call(
            write_kernel,
            out_shape=(jax.ShapeDtypeStruct(*y_shape), whole, whole),
            in_specs=[vmem] * 3,
            out_specs=(hbm, hbm, hbm),
            scratch_shapes=[dma((2 * WRITES + 1,))],
            compiler_params=pltpu.CompilerParams(vmem_limit_bytes=1 << 20),
            name="write_results",
        )(y_turned, k_new, v_new)
        return y_turned.T, k_out, v_out

    return jax.shard_map(
        local_step,
        mesh=mesh,
        in_specs=(P("dp", None), P(None, "tp"), P(), P(), P("tp", None), cache_spec, cache_spec, P("dp")),
        out_specs=(P("dp", "tp"), cache_spec, cache_spec),
        check_vma=False,
    )
```

```python
import functools
import math

import jax
import jax.numpy as jnp
import numpy as np
from jax import lax
from jax.experimental import pallas as pl
from jax.experimental.pallas import tpu as pltpu
from jax.sharding import PartitionSpec as P

F32, BF16 = jnp.float32, jnp.bfloat16
MESH = pl.DeviceIdType.MESH
O_STEPS = 4
WRITES = 1
SUB = 8
VMEM_LIMIT = 55 << 20
FIRST_W = 0


def step_kernel(side, hidden, wq_turned, w_key, w_value, w_out, k_in, v_in, lengths, freq_in, y_out, k_buf, v_buf,
                lens, freq, lens_f, h_buf, wq_buf, wk_buf, wv_buf, wo_buf, w_buf, k_new, v_new,
                q_send, q_recv, q_rows, s_rows, p_rows, o_rows, o_buf, y_acc, y_send, y_recv,
                h_sem, small_sem, wo_sem, k_sem, v_sem,
                q_ssem, q_rsem, q_rsem_late, w_ssem, w_rsem, w_xsem, o_ssem, o_rsem, near_ssem, far_ssem, near_rsem, far_rsem):
    rows, seq, dim = k_in.shape
    half = dim // 2
    pack = rows // 2
    group = 2 * side * side
    heads = group // 2
    cols = w_buf.shape[1]
    me = lax.axis_index("tp")
    core = lax.rem(me, 2)
    chip = me // 2
    x = lax.rem(chip, side)
    y = chip // side

    def index(xx, yy, cc):
        return (lax.rem(yy, side) * side + lax.rem(xx, side)) * 2 + cc

    def remote(src, dst, ssem, rsem, target):
        return pltpu.make_async_remote_copy(src_ref=src, dst_ref=dst, send_sem=ssem, recv_sem=rsem,
                                            device_id={"tp": target}, device_id_type=MESH)

    def wait_recv(ref, rsem):
        remote(ref, ref, q_ssem, rsem, me).wait_recv()

    def wait_send(ref, ssem):
        remote(ref, ref, ssem, q_rsem, me).wait_send()

    block = rows * 2 * side
    ydest = [lax.rem(y + d, side) for d in (2, 1, 3, 0)]

    def h_part(yy):
        return pl.ds(pl.multiple_of(yy * block, block), block)

    small = [pltpu.make_async_copy(src, dst, small_sem.at[i]) for i, (src, dst) in enumerate(
        ((wq_turned, wq_buf), (lengths, lens), (w_key, wk_buf), (w_value, wv_buf), (freq_in, freq)))]
    h_copies = [pltpu.make_async_copy(hidden.at[h_part(yy)], h_buf.at[h_part(yy)], h_sem.at[i]) for i, yy in enumerate(ydest)]
    wo_copies = [pltpu.make_async_copy(w_out.at[:, pl.ds(i * cols, cols)], wo_buf.at[i], wo_sem.at[i]) for i in range(side)]
    step_rows = rows // O_STEPS
    kv_copies = []
    for k in range(O_STEPS):
        part = pl.ds(k * step_rows, step_rows)
        kv_copies.append((pltpu.make_async_copy(k_in.at[part], k_buf.at[part], k_sem.at[k]),
                          pltpu.make_async_copy(v_in.at[part], v_buf.at[part], v_sem.at[k])))
    order = (0, 2, 1, 3)
    small[0].start()
    h_copies[0].start()

    barrier = pltpu.get_barrier_semaphore()
    peers = [(lax.rem(chip + i, heads)) * 2 + c for i in range(1, heads) for c in range(2)] + [chip * 2 + (1 - core)]
    for peer in peers:
        pl.semaphore_signal(barrier, inc=1, device_id={"tp": peer}, device_id_type=MESH)
    for copy in wo_copies + [h_copies[1], small[1], small[4]]:
        copy.start()

    def w_row(t):
        return (lax.rem(t, 2) * heads + t // 2) * half

    def w_slot(t):
        return w_buf.at[pl.ds(pl.multiple_of(w_row(t), half), half)]

    left, right, other = index(x + side - 1, y, core), index(x + 1, y, core), chip * 2 + (1 - core)
    n_w = [0]

    def send_w(src, t, target, first=0, size=None):
        size = half if size is None else size
        some = pl.ds(first, size)
        n_w[0] += size
        remote(src.at[some], w_slot(t).at[some], w_ssem, w_rsem.at[t], target).start()

    def give_w(src, t):
        n_w[0] += half
        remote(src, w_slot(t), w_ssem, w_xsem, other).start()

    def wait_w(t):
        wait_recv(w_slot(t), w_rsem.at[t])

    def first_w():
        for copy in wo_copies:
            copy.wait()
        for d in (1, 3, 2):
            send_w(wo_buf.at[lax.rem(y + d, side)], me, index(x, y + d, core))

    def own_w():
        for target in (right, left):
            send_w(wo_buf.at[y], me, target)
        give_w(wo_buf.at[y], me)
        w_buf[pl.ds(pl.multiple_of(w_row(me), half), half)] = wo_buf[y]

    with jax.named_scope("wait_wq"):
        small[0].wait()
    wq = wq_buf[...].T
    own = x * 2 + core
    quarter = pack // 2

    def send_q(i, part, rsem):
        some = pl.ds(part * quarter, quarter)
        slots = [lax.rem(x + d, side) * 2 + c for d in (2, 1, 3) for c in range(2)] + [x * 2 + 1 - core]
        for slot in slots + ([own] if i < side - 1 else []):
            remote(q_send.at[i * 2 * side + slot, some], q_recv.at[me, some], q_ssem, rsem, ydest[i] * 2 * side + slot).start()

    for i, yy in enumerate(ydest):
        with jax.named_scope("wait_h"):
            h_copies[i].wait()
        if i + 2 < side:
            h_copies[i + 2].start()
        if i == 1:
            for copy in small[2:4]:
                copy.start()
        if i == 2:
            for k in order[:2]:
                for copy in kv_copies[k]:
                    copy.start()
        for part in range(2):
            some = pl.ds(pl.multiple_of(yy * block + part * (block // 2), block // 2), block // 2)
            q_val = jnp.dot(h_buf[some, :], wq, preferred_element_type=F32).astype(BF16)
            q_val = q_val.reshape(side, 2, pack, half)
            q_send[pl.ds(i * 2 * side + part * side, side)] = jnp.concatenate([q_val[:, 0], q_val[:, 1]], axis=-1)
        if i == 0:
            with jax.named_scope("barrier"):
                pl.semaphore_wait(barrier, len(peers))

        send_q(i, 0, q_rsem)
        if i == FIRST_W:
            first_w()
    own_w()
    for i in range(side):
        send_q(i, 1, q_rsem_late)
    q_recv[me] = q_send[(side - 1) * 2 * side + own]
    for k in order[2:]:
        for copy in kv_copies[k]:
            copy.start()

    def forward_column(d):
        t = index(x, y + d, core)
        wait_w(t)
        for target in (left, right):
            send_w(w_slot(t), t, target)
        give_w(w_slot(t), t)

    def relay_right(d):
        t = index(x + side - 1, y + d, core)
        wait_w(t)
        send_w(w_slot(t), t, right)
        give_w(w_slot(t), t)

    def relay_both(d):
        for xx, target, first in ((x + 1, left, 0), (x + side - 1, right, half // 2)):
            t = index(xx, y + d, core)
            wait_w(t)
            send_w(w_slot(t), t, target, first, half // 2)
            give_w(w_slot(t), t)

    def relay_left(d):
        t = index(x + 1, y + d, core)
        wait_w(t)
        send_w(w_slot(t), t, left)
        give_w(w_slot(t), t)

    def pass_on(xx, d):
        t = index(xx, y + d, core)
        wait_w(t)
        give_w(w_slot(t), t)

    with jax.named_scope("tables"):
        small[1].wait()
        small[4].wait()

        def spread(r, carry):
            lens_f[pl.ds(r, 1), :] = jnp.full((1, dim), lens[me * rows + r].astype(F32))
            return carry

        lax.fori_loop(0, rows, spread, 0, unroll=8)
        angles = lens_f[...] * freq[...]
        cos, sin = jnp.cos(angles), jnp.sin(angles)
        low = lax.broadcasted_iota(jnp.int32, (rows, dim), 1) < half
        low_pack = lax.broadcasted_iota(jnp.int32, (pack, dim), 1) < half
        c_pack = jnp.where(low_pack, cos[:pack], cos[pack:])
        s_pack = jnp.where(low_pack, sin[:pack], sin[pack:])
        small[2].wait()
        small[3].wait()
        h_own = h_buf[pl.ds(pl.multiple_of(me * rows, rows), rows), :]
        key = jnp.dot(h_own, wk_buf[...], preferred_element_type=F32).astype(BF16).astype(F32)
        turned_key = pltpu.roll(key, half, 1)
        k_new[...] = jnp.where(low, key * cos - turned_key * sin, key * cos + turned_key * sin)
        v_new[...] = jnp.dot(h_own, wv_buf[...], preferred_element_type=F32)
    slot_rows = lax.broadcasted_iota(jnp.int32, (seq, dim), 0).astype(F32).astype(BF16)

    def patch(k):
        for copy in kv_copies[k]:
            copy.wait()

        def patch_row(j, carry):
            r = k * step_rows + j
            here = slot_rows == lens_f[pl.ds(r, 1), :].astype(BF16)
            k_buf[r] = jnp.where(here, k_new[pl.ds(r, 1), :].astype(BF16), k_buf[r])
            v_buf[r] = jnp.where(here, v_new[pl.ds(r, 1), :].astype(BF16), v_buf[r])
            return carry

        lax.fori_loop(0, step_rows, patch_row, 0)

    with jax.named_scope("patch"):
        for k in order:
            patch(k)
    with jax.named_scope("column"):
        for d in (1, 3, 2):
            forward_column(d)

    def wait_q(part, rsem):
        wait_recv(q_recv.at[pl.ds(0, group - 1), pl.ds(part * quarter, quarter)], rsem)

    low_quarter = lax.broadcasted_iota(jnp.int32, (quarter, dim), 1) < half

    def rope(part):
        span = pl.ds(part * quarter, quarter)
        c_part, s_part = c_pack[part * quarter:(part + 1) * quarter], s_pack[part * quarter:(part + 1) * quarter]
        for i in range(heads):
            p1, p2 = q_recv[2 * i, span, :].astype(F32), q_recv[2 * i + 1, span, :].astype(F32)
            r1, r2 = p1 * c_part - p2 * s_part, p2 * c_part + p1 * s_part
            at = part * quarter * heads + i
            q_rows[pl.ds(at, quarter, stride=heads), :] = jnp.where(low_quarter, r1, pltpu.roll(r2, half, 1))
            q_rows[pl.ds(pack * heads + at, quarter, stride=heads), :] = jnp.where(low_quarter, pltpu.roll(r1, half, 1), r2)

    scale = dim ** -0.5
    slots = lax.broadcasted_iota(jnp.int32, (heads, seq), 1).astype(F32)
    up, down = index(x, y + 1, core), index(x, y + side - 1, core)
    y_up, y_down, y_far = lax.rem(y + 1, side), lax.rem(y + side - 1, side), lax.rem(y + 2, side)

    def send_o(yy, k, target, some=slice(None)):
        piece = o_buf.at[yy * O_STEPS + k, some]
        remote(piece, piece, o_ssem, o_rsem.at[yy, k], target).start()

    def wait_o(yy, k):
        wait_recv(o_buf.at[yy * O_STEPS + k], o_rsem.at[yy, k])

    def relay_o(k):
        wait_o(y_down, k)
        send_o(y_down, k, up, pl.ds(0, heads // 2))
        wait_o(y_up, k)
        send_o(y_up, k, down, pl.ds(heads // 2, heads // 2))

    def score(k, part):
        r = k * step_rows + part
        q_row = q_rows[pl.ds(r * heads, heads), :].astype(BF16)
        scores = lax.dot_general(q_row, k_buf[r], (((1,), (1,)), ((), ())), preferred_element_type=F32) * scale
        last = jnp.concatenate([lens_f[pl.ds(r, 1), :]] * (seq // dim), axis=1)
        s_rows[pl.ds(part * heads, heads), :] = jnp.where(slots <= last, scores, -1e30)

    low_step = lax.broadcasted_iota(jnp.int32, (step_rows, dim), 1) < half

    def attend(k):
        for part in range(step_rows):
            score(k, part)
        for first in range(0, step_rows, SUB):
            span = pl.ds(first * heads, SUB * heads)
            scores = s_rows[span, :]
            weights = jnp.exp(scores - jnp.max(scores, axis=1, keepdims=True))
            p_rows[span, :] = weights.astype(BF16)
            total = jnp.sum(weights, axis=1, keepdims=True)
            for u in range(SUB):
                part = first + u
                summed = jnp.dot(p_rows[pl.ds(part * heads, heads), :], v_buf[k * step_rows + part], preferred_element_type=F32)
                o_rows[pl.ds(part * heads, heads), :] = summed / total[u * heads:(u + 1) * heads]
        for i in range(heads // 2):
            even, odd = (o_rows[pl.ds(2 * i + j, step_rows, stride=heads), :] for j in range(2))
            o_buf[y * O_STEPS + k, i] = jnp.where(low_step, even, pltpu.roll(odd, half, 1)).astype(BF16)
            o_buf[y * O_STEPS + k, heads // 2 + i] = jnp.where(low_step, pltpu.roll(even, half, 1), odd).astype(BF16)
        send_o(y, k, up)
        send_o(y, k, down)

    with jax.named_scope("wait_q"):
        wait_q(0, q_rsem)
    with jax.named_scope("attend0"):
        rope(0)
        attend(0)
    with jax.named_scope("relay0"):
        relay_right(0)
        pass_on(x + 1, 0)
    with jax.named_scope("attend1"):
        attend(2)
    with jax.named_scope("wait_q_late"):
        wait_q(1, q_rsem_late)
    with jax.named_scope("attend2"):
        rope(1)
        attend(1)
        attend(3)
    with jax.named_scope("relay2"):
        relay_right(1)
        relay_left(3)
        relay_both(2)
    with jax.named_scope("relay3"):
        relay_o(0)
        pass_on(x + side - 1, 3)
        pass_on(x + 1, 1)
    with jax.named_scope("relay4"):
        relay_o(2)
        relay_o(1)
    with jax.named_scope("relay5"):
        relay_o(3)
    with jax.named_scope("wait_w_far"):
        for d in (0, 1, 3, 2):
            pass_on(x + 2, d)
    sources = [y, y_up, y_down, y_far]
    near = side - 1
    depth = heads * half

    def row_peers():
        return [lax.rem(x + d, side) * 2 + c for d in (2, 1, 3) for c in range(2)] + [x * 2 + 1 - core]

    def partial(some, c):
        lhs = [jnp.concatenate([o_buf[pl.ds(sources[n] * O_STEPS, O_STEPS), c * (heads // 2) + i].reshape(rows, dim)
                                for i in range(heads // 2)], axis=1) for n in some]
        return jnp.dot(jnp.concatenate(lhs, axis=0), w_buf[pl.ds(pl.multiple_of(c * depth, depth), depth), :],
                       preferred_element_type=F32)

    def place(some, res):
        for m, n in enumerate(some):
            for slot in range(0, 2 * side, 2):
                turned = res[m * rows:(m + 1) * rows, slot * half:(slot + 2) * half].T.astype(BF16)
                for c in range(2):
                    part = turned[c * half:(c + 1) * half]
                    y_send[slot + c, n] = jnp.concatenate([part[:half // 2], part[half // 2:]], axis=1)

    with jax.named_scope("near_own"):
        y_acc[...] = partial(range(near), core)
    with jax.named_scope("wait_w_other"):
        wait_recv(w_buf.at[pl.ds(0, depth)], w_xsem)
    with jax.named_scope("near_other"):
        place(range(near), y_acc[...] + partial(range(near), 1 - core))
        for slot in row_peers():
            remote(y_send.at[slot, pl.ds(0, near)], y_recv.at[own, pl.ds(0, near)], near_ssem, near_rsem, y * 2 * side + slot).start()
    with jax.named_scope("wait_o_far"):
        for k in range(O_STEPS):
            wait_o(y_far, k)
    with jax.named_scope("project_far"):
        place([near], partial([near], core) + partial([near], 1 - core))
        for slot in row_peers():
            remote(y_send.at[slot, near], y_recv.at[own, near], far_ssem, far_rsem, y * 2 * side + slot).start()
        y_recv[own] = y_send[own]

    def finish(n):
        for i in range(side):
            a, b = y_recv[2 * i, n], y_recv[2 * i + 1, n]
            span = pl.ds(pl.multiple_of((sources[n] * side + i) * 2 * rows, 2 * rows), 2 * rows)
            y_out[pl.ds(0, half // 2), span] = jnp.concatenate([a[:, :rows], b[:, :rows]], axis=1)
            y_out[pl.ds(half // 2, half // 2), span] = jnp.concatenate([a[:, rows:], b[:, rows:]], axis=1)

    others = pl.ds(0, 2 * side - 1)
    with jax.named_scope("drain"):
        wait_send(q_send.at[pl.ds(0, group - 1)], q_ssem)
        wait_send(w_buf.at[pl.ds(0, n_w[0])], w_ssem)
        wait_send(o_buf.at[pl.ds(0, 3 * O_STEPS)], o_ssem)
        wait_send(y_send.at[others, pl.ds(0, near)], near_ssem)
    with jax.named_scope("wait_y_near"):
        wait_recv(y_recv.at[others, pl.ds(0, near)], near_rsem)
    for n in range(near):
        finish(n)
    with jax.named_scope("wait_y_far"):
        wait_recv(y_recv.at[others, near], far_rsem)
    finish(near)
    wait_send(y_send.at[others, near], far_ssem)


def write_kernel(y_in, k_in, v_in, y_out, k_out, v_out, sems):
    rows = k_in.shape[0]
    part_rows = rows // WRITES
    copies = []
    for src, dst in ((k_in, k_out), (v_in, v_out)):
        for j in range(WRITES):
            part = pl.ds(j * part_rows, part_rows)
            copies.append(pltpu.make_async_copy(src.at[part], dst.at[part], sems.at[len(copies)]))
    copies.append(pltpu.make_async_copy(y_in, y_out, sems.at[len(copies)]))
    for copy in copies:
        copy.start()
    for copy in copies:
        copy.wait()


def solution(mesh):
    group = mesh.shape["tp"]
    side = math.isqrt(group // 2)
    cache_spec = P(("dp", "tp"), None, None)
    vmem, hbm = pl.BlockSpec(memory_space=pltpu.VMEM), pl.BlockSpec(memory_space=pltpu.HBM)
    dma = pltpu.SemaphoreType.DMA

    def local_step(hidden, w_query, w_key, w_value, w_out, k_cache, v_cache, lengths):
        rows, seq, dim = k_cache.shape
        batch, embed = hidden.shape
        half = dim // 2
        heads = group * w_query.shape[1] // dim
        cols = w_out.shape[1] // side
        freq = (10000.0 ** (-(np.arange(half) * 2.0) / dim)).astype(np.float32)
        freq = jnp.asarray(np.concatenate([freq, freq])[None, :])
        cache_shape = pltpu.VMEM(k_cache.shape, k_cache.dtype)
        packed = pltpu.VMEM((2 * side, side, half // 2, dim), BF16)
        y_shape = ((w_out.shape[1] // group, batch), BF16)
        y_turned, k_new, v_new = pl.pallas_call(
            functools.partial(step_kernel, side),
            out_shape=(pltpu.VMEM(*y_shape), cache_shape, cache_shape),
            in_specs=[hbm] * 9,
            out_specs=(vmem, vmem, vmem),
            scratch_shapes=[
                pltpu.SMEM((batch,), jnp.int32), pltpu.VMEM((1, dim), F32), pltpu.VMEM((rows, dim), F32),
                pltpu.VMEM((batch, embed), BF16), pltpu.VMEM((half, embed), BF16),
                pltpu.VMEM((embed, dim), BF16), pltpu.VMEM((embed, dim), BF16),
                pltpu.VMEM((side, half, cols), BF16), pltpu.VMEM((group * half, cols), BF16),
                pltpu.VMEM((rows, dim), F32), pltpu.VMEM((rows, dim), F32),
                pltpu.VMEM((group, rows // 2, dim), BF16), pltpu.VMEM((group, rows // 2, dim), BF16),
                pltpu.VMEM((rows * heads, dim), F32), pltpu.VMEM((rows // O_STEPS * heads, seq), F32),
                pltpu.VMEM((rows // O_STEPS * heads, seq), BF16), pltpu.VMEM((rows // O_STEPS * heads, dim), F32),
                pltpu.VMEM((side * O_STEPS, heads, rows // O_STEPS, dim), BF16),
                pltpu.VMEM(((side - 1) * rows, cols), F32), packed, packed,
                dma((side,)), dma((5,)), dma((side,)), dma((O_STEPS,)), dma((O_STEPS,)),
                dma, dma, dma, dma, dma((group,)), dma, dma, dma((side, O_STEPS)), dma, dma, dma, dma,
            ],
            compiler_params=pltpu.CompilerParams(collective_id=0, has_side_effects=True, vmem_limit_bytes=VMEM_LIMIT),
            name="attention_step",
        )(hidden, w_query.T, w_key, w_value, w_out, k_cache, v_cache, lengths, freq)
        whole = jax.ShapeDtypeStruct(k_cache.shape, k_cache.dtype)
        y_turned, k_out, v_out = pl.pallas_call(
            write_kernel,
            out_shape=(jax.ShapeDtypeStruct(*y_shape), whole, whole),
            in_specs=[vmem] * 3,
            out_specs=(hbm, hbm, hbm),
            scratch_shapes=[dma((2 * WRITES + 1,))],
            compiler_params=pltpu.CompilerParams(vmem_limit_bytes=1 << 20),
            name="write_results",
        )(y_turned, k_new, v_new)
        return y_turned.T, k_out, v_out

    return jax.shard_map(
        local_step,
        mesh=mesh,
        in_specs=(P("dp", None), P(None, "tp"), P(), P(), P("tp", None), cache_spec, cache_spec, P("dp")),
        out_specs=(P("dp", "tp"), cache_spec, cache_spec),
        check_vma=False,
    )
```
